128 devices in a mesh: blk: 128 (over z, x, y, core).
Axes of the slice: x: 4, y: 4, z: 4, core: 2. Of those that a mesh axis runs over, the one named last changes fastest.
Arguments:
- tokens: bfloat16 [65536, 1024], P('blk'), may hold values from -6 to 6
- labels: bfloat16 [65536, 1024], P('blk'), may hold values from -192 to 192
- lengths: int32 [256], P('blk'), may hold values from 1 to 256, as said below
- targets: int32 [65536], P('blk'), may hold values 0 or 1
- w_in: bfloat16 [1024, 2560], replicated, may hold values from -0.1875 to 0.1875
- b_in: float32 [2560], replicated, may hold values from -3 to 3
- w_out: bfloat16 [1024, 1024], replicated, may hold values from -0.1875 to 0.1875
Outputs:
- layer_out: bfloat16 [65536, 1024], P('blk')
- loss: float32 [], replicated
- grad_tokens: bfloat16 [65536, 1024], P('blk')
- grad_in: bfloat16 [1024, 2560], replicated
- grad_bias: float32 [2560], replicated
- grad_out: bfloat16 [1024, 1024], replicated
The draws below stay inside these ranges and needn't reach their ends.
Inputs may be any that keep to these rules, and one draw needn't show every extreme that they name: `lengths`: some history has exactly 256 used rows.
All inputs are finite; a program needn't handle non-finite values. No bound on the sum of `targets` on one device may be relied on, other than what follows from the above.
Results may differ from the reference program's by a relative error of at most 0.015.
Values may be sent and summed in bfloat16 or wider, within the bound.
No kernel may reach another device: no remote copies, remote signals or barrier semaphores. Data moves between devices by JAX's collectives and lax.ppermute only.
A program may use at most 128 MiB of HBM per device.

```python
from functools import partial
import jax
import jax.numpy as jnp
from jax import lax

D = 1024
HEADS = 4
VDIM = 256
QKDIM = 64
LMAX = 256
COLS = 2560
HISTS = 256
TOKENS = 65536
N_BLK = 128


def draw_lengths(key, part):
    first, second, third = jax.random.split(jax.random.fold_in(key, 7), 3)
    drawn_one = jax.random.randint(first, (HISTS,), 1, LMAX + 1)
    drawn_two = jax.random.randint(second, (HISTS,), 1, LMAX + 1)
    drawn = jnp.minimum(drawn_one, drawn_two)
    picked = jax.random.randint(third, (), 0, HISTS)
    return jnp.where(lax.iota(jnp.int32, HISTS) == picked, LMAX, drawn).astype(jnp.int32)


def set_ends(result, rng, low, high):
    longest = result.shape.index(max(result.shape))
    spots = []
    for shift in (0, 1):
        where = [jax.random.randint(jax.random.fold_in(rng, axis), (), 0, length) for axis, length in enumerate(result.shape)]
        where[longest] = (where[longest] + shift) % result.shape[longest]
        spots.append(tuple(where))
    return result.at[spots[0]].set(low).at[spots[1]].set(high)


def steps_of(key, dims, shards, low, largest):
    factor_of, own = 1.0, jax.random.fold_in(key, 6)
    for dim, parts in shards:
        draws = jnp.exp(jax.random.uniform(jax.random.fold_in(own, dim), (parts,), jnp.float32, low / len(shards), largest / len(shards)))
        factor_of = factor_of * jnp.repeat(draws, dims[dim] // parts).reshape([-1 if axis == dim else 1 for axis in range(len(dims))])
    return factor_of


def normal_values(rng, dims, scale, bound, cuts=(), kind=jnp.bfloat16):
    values = scale * jax.random.normal(rng, dims, jnp.float32)
    if cuts:
        values = values * steps_of(rng, dims, cuts, -0.22, 0.18)
    return jnp.clip(values, -bound, bound).astype(kind)


def setup_inputs(seed: int = 0) -> dict:
    splits = jax.random.split(jax.random.key(seed), 8)
    tokens = normal_values(splits[0], (TOKENS, D), 1.0, 6.0, ((0, 128),))
    labels = normal_values(splits[1], (TOKENS, D), 32.0, 192.0, ((0, 128),))
    lengths = draw_lengths(jax.random.fold_in(splits[7], 71), 0)
    targets = set_ends((jax.random.randint(splits[3], (TOKENS,), 0, 8) < 1).astype(jnp.int32), jax.random.fold_in(splits[3], 1), 0, 1)
    w_in = normal_values(splits[4], (D, COLS), D ** -0.5, 0.1875)
    b_in = normal_values(splits[5], (COLS,), 0.5, 3.0, (), jnp.float32)
    w_out = normal_values(splits[6], (HEADS * VDIM, D), (HEADS * VDIM) ** -0.5, 0.1875)
    return dict(tokens=tokens, labels=labels, lengths=lengths, targets=targets, w_in=w_in, b_in=b_in, w_out=w_out)


EPS = 1e-05

def norm_rows(values):
    center = values - lax.optimization_barrier(jnp.mean(values, axis=-1, keepdims=True))
    spread = lax.optimization_barrier(jnp.mean(center * center, axis=-1, keepdims=True))
    return center * lax.rsqrt(spread + EPS)

def history_layer(rows, length, w_in, b_in, w_out):
    count_rows = rows.shape[0]
    normed = norm_rows(rows).astype(jnp.bfloat16)
    hidden = jnp.dot(normed, w_in, preferred_element_type=jnp.float32) + b_in
    acts = jax.nn.silu(hidden).astype(jnp.bfloat16)
    width = HEADS * VDIM
    gate = acts[:, :width]
    values = acts[:, width:2 * width].reshape(count_rows, HEADS, VDIM).astype(jnp.float32)
    queries = acts[:, 2 * width:2 * width + HEADS * QKDIM].reshape(count_rows, HEADS, QKDIM).astype(jnp.float32)
    keys = acts[:, 2 * width + HEADS * QKDIM:].reshape(count_rows, HEADS, QKDIM).astype(jnp.float32)
    places = lax.iota(jnp.int32, count_rows)
    allowed = (places[None, :] <= places[:, None]) & (places[None, :] < length)
    scores = jnp.einsum('qhe,khe->hqk', queries, keys)
    weights = jnp.where(allowed[None], jax.nn.silu(scores), 0.0).astype(jnp.bfloat16)
    mixed = jnp.einsum('hqk,khe->qhe', weights.astype(jnp.float32), values).reshape(count_rows, width)
    gated = (norm_rows(mixed) * gate.astype(jnp.float32)).astype(jnp.bfloat16)
    full = rows + jnp.dot(gated, w_out, preferred_element_type=jnp.float32)
    return jnp.where((places < length)[:, None], full, 0.0)

def batch_layer(block, w_in, b_in, w_out, spans):
    return jax.vmap(history_layer, in_axes=(0, 0, None, None, None))(block, spans, w_in, b_in, w_out)

def reference(tokens, labels, lengths, targets, w_in, b_in, w_out):
    per_dev = HISTS // N_BLK
    rows = tokens.reshape(N_BLK, per_dev, LMAX, D).astype(jnp.float32)
    label_rows = labels.reshape(N_BLK, per_dev, LMAX, D).astype(jnp.float32)
    spans = lengths.reshape(N_BLK, per_dev)
    marks = targets.reshape(N_BLK, per_dev, LMAX)
    places = lax.iota(jnp.int32, LMAX)

    def one_device(carry, item):
        block, label_block, span_block, mark_block = item
        used = places[None, :] < span_block[:, None]
        chosen = ((mark_block == 1) | (places[None, :] == span_block[:, None] - 1)) & used
        full, pullback = jax.vjp(partial(batch_layer, spans=span_block), block, w_in, b_in, w_out)
        cot = jnp.where(chosen[..., None], label_block, 0.0)
        d_rows, d_in, d_bias, d_out = pullback(cot)
        rounded = full.astype(jnp.bfloat16)
        loss_part = jnp.sum(cot * rounded.astype(jnp.float32))
        count_part = jnp.sum(chosen.astype(jnp.float32))
        sum_in, sum_bias, sum_out, sum_loss, sum_count = carry
        carry = (sum_in + d_in.astype(jnp.float32), sum_bias + d_bias, sum_out + d_out.astype(jnp.float32), sum_loss + loss_part, sum_count + count_part)
        return (carry, (rounded, d_rows))
    start = (jnp.zeros((D, COLS), jnp.float32), jnp.zeros((COLS,), jnp.float32), jnp.zeros((HEADS * VDIM, D), jnp.float32), jnp.zeros((), jnp.float32), jnp.zeros((), jnp.float32))
    totals, stacked = lax.scan(one_device, start, (rows, label_rows, spans, marks))
    sum_in, sum_bias, sum_out, sum_loss, total = totals
    outputs, d_rows = stacked
    layer_out = outputs.reshape(TOKENS, D)
    grad_tokens = (d_rows / total).astype(jnp.bfloat16).reshape(TOKENS, D)
    return (layer_out, sum_loss / total, grad_tokens, (sum_in / total).astype(jnp.bfloat16), sum_bias / total, (sum_out / total).astype(jnp.bfloat16))
```

```python
import functools

import jax
import jax.numpy as jnp
from jax import lax
from jax.experimental import pallas as pl
from jax.experimental.pallas import tpu as pltpu
from jax.sharding import Mesh
from jax.sharding import PartitionSpec as P

D = 1024
HEADS = 4
VDIM = 256
QKDIM = 64
LMAX = 256
COLS = 2560
ROWS = 512
QCOL = 2048
KCOL = 2304
AXES = ("z", "x", "y", "c")
CHIPS = ("z", "x", "y")
PIECES = 64
BLOCKS = 14
DATA = BLOCKS * 16
PIECE = DATA + 8
EPS = 1e-05
F32 = jnp.float32
BF16 = jnp.bfloat16
INTERPRET = False


def sigmoid(h):
    return 0.5 * jnp.tanh(0.5 * h) + 0.5


def nn(a, b):
    return jnp.dot(a, b, preferred_element_type=F32)


def nt(a, b):
    return lax.dot_general(a, b, (((1,), (1,)), ((), ())), preferred_element_type=F32)


def tn(a, b):
    return lax.dot_general(a, b, (((0,), (0,)), ((), ())), preferred_element_type=F32)


def three_parts(value):
    hi = value.astype(BF16).astype(F32)
    rest = value - hi
    mid = rest.astype(BF16).astype(F32)
    low = (rest - mid).astype(BF16).astype(F32)
    return hi, mid, low


def row_stats(x):
    center = x - jnp.mean(x, axis=-1, keepdims=True)
    spread = jnp.mean(center * center, axis=-1, keepdims=True)
    return center, lax.rsqrt(spread + EPS)


def allowed_mask(length):
    i = lax.broadcasted_iota(jnp.int32, (LMAX, LMAX), 0)
    j = lax.broadcasted_iota(jnp.int32, (LMAX, LMAX), 1)
    return (j <= i) & (j < length)


def local_kernel(
    meta, tgt, tok, lab, win, bias, wout,
    out, dx, mine, send,
    hid, normed, normed_t, acts, dh, mixed, gated_t, dm, sc, wt, cot, inv_s, dqk, bsum, lsum, csum, ext, pay, sems,
):
    core = meta[2]
    bsum[...] = jnp.zeros_like(bsum)
    lsum[...] = jnp.zeros_like(lsum)
    csum[...] = jnp.zeros_like(csum)

    def prologue(r, carry):
        rows = pl.ds(pl.multiple_of(r * 128, 128), 128)
        length = meta[r // 2]
        place = (r % 2) * 128 + lax.broadcasted_iota(jnp.int32, (128, 128), 0)
        marks = jnp.transpose(jnp.broadcast_to(tgt[pl.ds(r, 1), :].astype(F32), (128, 128)))
        chosen = ((marks == 1.0) | (place == length - 1)) & (place < length)
        flag = jnp.where(chosen, 1.0, 0.0)
        csum[...] += jnp.sum(flag, axis=0, keepdims=True)
        wide = jnp.concatenate([flag] * 8, axis=1)
        cot[rows, :] = jnp.where(wide > 0.0, lab[rows, :].astype(F32), 0.0).astype(BF16)
        center, inv = row_stats(tok[rows, :].astype(F32))
        y = center * inv
        normed[rows, :] = y.astype(BF16)
        normed_t[:, rows] = jnp.transpose(y).astype(BF16)
        return carry

    lax.fori_loop(0, 4, prologue, 0)

    def project(c, carry):
        cols = pl.ds(pl.multiple_of(c * 512, 512), 512)
        h = nn(normed[...], win[:, cols]) + bias[:, cols]
        hid[:, cols] = h
        acts[:, cols] = (h * sigmoid(h)).astype(BF16)
        return carry

    lax.fori_loop(0, 5, project, 0)

    for n in range(2):
        rows = slice(n * LMAX, (n + 1) * LMAX)
        allowed = allowed_mask(meta[n])
        for h in range(HEADS):
            q = acts[rows, QCOL + h * QKDIM : QCOL + (h + 1) * QKDIM]
            k = acts[rows, KCOL + h * QKDIM : KCOL + (h + 1) * QKDIM]
            v = acts[rows, D + h * VDIM : D + (h + 1) * VDIM]
            s = nt(q, k)
            w = jnp.where(allowed, s * sigmoid(s), 0.0).astype(BF16)
            sc[n * HEADS + h] = s
            wt[n * HEADS + h] = w
            mixed[rows, h * VDIM : (h + 1) * VDIM] = nn(w, v)

    def gate(r, carry):
        rows = pl.ds(pl.multiple_of(r * 128, 128), 128)
        center, inv = row_stats(mixed[rows, :])
        y = center * inv
        mixed[rows, :] = y
        inv_s[rows, :] = jnp.broadcast_to(inv, (128, 128))
        gated = (y * acts[rows, :D].astype(F32)).astype(BF16)
        gated_t[:, rows] = jnp.transpose(gated.astype(F32)).astype(BF16)
        length = meta[r // 2]
        place = (r % 2) * 128 + lax.broadcasted_iota(jnp.int32, (128, D), 0)
        full = tok[rows, :].astype(F32) + nn(gated, wout[...])
        rounded = jnp.where(place < length, full, 0.0).astype(BF16)
        out[rows, :] = rounded
        c = cot[rows, :]
        lsum[...] += jnp.sum(c.astype(F32) * rounded.astype(F32), axis=0, keepdims=True)
        dg = nt(c, wout[...]).astype(BF16).astype(F32)
        u = acts[rows, :D].astype(F32)
        dy = dg * u
        du = (dg * y).astype(BF16).astype(F32)
        m1 = jnp.mean(dy, axis=-1, keepdims=True)
        m2 = jnp.mean(dy * y, axis=-1, keepdims=True)
        dm[rows, :] = (inv * (dy - m1 - y * m2)).astype(BF16)
        hu = hid[rows, :D]
        sg = sigmoid(hu)
        dhu = du * (sg * (1.0 + hu * (1.0 - sg)))
        dh[rows, :D] = dhu.astype(BF16)
        bsum[0:1, :D] += jnp.sum(dhu, axis=0, keepdims=True)
        return carry

    lax.fori_loop(0, 4, gate, 0)

    def store(j, value):
        half, jj = j // BLOCKS, j % BLOCKS
        pay[half, :, jj * 16 : (jj + 1) * 16, :] = value.astype(BF16).reshape(PIECES, 16, 128)

    for c in range(2):
        g = nn(gated_t[...], cot[:, c * 512 : (c + 1) * 512])
        for i in range(4):
            store(20 + 4 * c + i, g[:, i * 128 : (i + 1) * 128])

    for n in range(2):
        rows = slice(n * LMAX, (n + 1) * LMAX)
        allowed = allowed_mask(meta[n])
        for h in range(HEADS):
            q = acts[rows, QCOL + h * QKDIM : QCOL + (h + 1) * QKDIM]
            k = acts[rows, KCOL + h * QKDIM : KCOL + (h + 1) * QKDIM]
            vc = slice(D + h * VDIM, D + (h + 1) * VDIM)
            d = dm[rows, h * VDIM : (h + 1) * VDIM]
            dw = nt(d, acts[rows, vc]).astype(BF16).astype(F32)
            dv = tn(wt[n * HEADS + h], d).astype(BF16).astype(F32)
            s = sc[n * HEADS + h]
            sg = sigmoid(s)
            ds = jnp.where(allowed, dw * (sg * (1.0 + s * (1.0 - sg))), 0.0).astype(BF16)
            dqk[rows, h * QKDIM : (h + 1) * QKDIM] = nn(ds, k)
            dqk[rows, 256 + h * QKDIM : 256 + (h + 1) * QKDIM] = tn(ds, q)
            hv = hid[rows, vc]
            sg = sigmoid(hv)
            dhv = dv * (sg * (1.0 + hv * (1.0 - sg)))
            dh[rows, vc] = dhv.astype(BF16)
            bsum[0:1, vc] += jnp.sum(dhv, axis=0, keepdims=True)
        hq = hid[rows, QCOL:]
        sg = sigmoid(hq)
        dhq = dqk[rows, :].astype(BF16).astype(F32) * (sg * (1.0 + hq * (1.0 - sg)))
        dh[rows, QCOL:] = dhq.astype(BF16)
        bsum[0:1, QCOL:] += jnp.sum(dhq, axis=0, keepdims=True)

    for c in range(5):
        g = nn(normed_t[...], dh[:, c * 512 : (c + 1) * 512])
        for i in range(4):
            store(4 * c + i, g[:, i * 128 : (i + 1) * 128])

    ext[...] = jnp.zeros_like(ext)
    for j in range(COLS // 128):
        parts = three_parts(bsum[0:1, j * 128 : (j + 1) * 128])
        base = 8 * (j // 2) + j % 2
        for t in range(3):
            ext[base + 2 * t : base + 2 * t + 1, :] = parts[t]
    loss = jnp.sum(lsum[...], axis=1, keepdims=True)
    lane = lax.broadcasted_iota(jnp.int32, (1, 128), 1)
    tail = jnp.where(lane == 0, jnp.broadcast_to(loss, (1, 128)), jnp.where(lane == 1, csum[...], 0.0))
    parts = three_parts(tail)
    for t in range(3):
        ext[80 + 2 * t : 81 + 2 * t, :] = parts[t]
    for half in range(2):
        pay[half, :, DATA:, :] = jnp.zeros((PIECES, 8, 128), BF16)
        for p in range(11):
            pay[half, p, DATA:, :] = ext[8 * p : 8 * p + 8, :].astype(BF16)

    to_send = pltpu.make_async_copy(pay.at[1 - core], send, sems.at[0])
    to_keep = pltpu.make_async_copy(pay.at[core], mine, sems.at[1])
    to_send.start()
    to_keep.start()

    def back(r, carry):
        rows = pl.ds(pl.multiple_of(r * 128, 128), 128)
        dn = nt(dh[rows, :], win[...]).astype(BF16).astype(F32)
        center, inv = row_stats(tok[rows, :].astype(F32))
        y = center * inv
        m1 = jnp.mean(dn, axis=-1, keepdims=True)
        m2 = jnp.mean(dn * y, axis=-1, keepdims=True)
        dx[rows, :] = inv * (dn - m1 - y * m2) + cot[rows, :].astype(F32)
        return carry

    lax.fori_loop(0, 4, back, 0)
    to_send.wait()
    to_keep.wait()


def local_step(meta, tgt, tok, lab, win, bias, wout):
    vm = pl.BlockSpec(memory_space=pltpu.VMEM)
    hbm = pl.BlockSpec(memory_space=pl.ANY)
    half = jax.ShapeDtypeStruct((PIECES, PIECE, 128), BF16)
    return pl.pallas_call(
        local_kernel,
        in_specs=[pl.BlockSpec(memory_space=pltpu.SMEM)] + [vm] * 6,
        out_specs=[vm, vm, hbm, hbm],
        out_shape=[
            jax.ShapeDtypeStruct((ROWS, D), BF16),
            jax.ShapeDtypeStruct((ROWS, D), F32),
            half,
            half,
        ],
        scratch_shapes=[
            pltpu.VMEM((ROWS, COLS), F32),
            pltpu.VMEM((ROWS, D), BF16),
            pltpu.VMEM((D, ROWS), BF16),
            pltpu.VMEM((ROWS, COLS), BF16),
            pltpu.VMEM((ROWS, COLS), BF16),
            pltpu.VMEM((ROWS, D), F32),
            pltpu.VMEM((D, ROWS), BF16),
            pltpu.VMEM((ROWS, D), BF16),
            pltpu.VMEM((2 * HEADS, LMAX, LMAX), F32),
            pltpu.VMEM((2 * HEADS, LMAX, LMAX), BF16),
            pltpu.VMEM((ROWS, D), BF16),
            pltpu.VMEM((ROWS, 128), F32),
            pltpu.VMEM((ROWS, 512), F32),
            pltpu.VMEM((8, COLS), F32),
            pltpu.VMEM((1, D), F32),
            pltpu.VMEM((1, 128), F32),
            pltpu.VMEM((88, 128), F32),
            pltpu.VMEM((2, PIECES, PIECE, 128), BF16),
            pltpu.SemaphoreType.DMA((2,)),
        ],
        compiler_params=pltpu.CompilerParams(vmem_limit_bytes=58 * 2**20),
        interpret=INTERPRET,
        name="local_step",
    )(meta, tgt, tok, lab, win, bias, wout)


def resplit(total):
    value = total[..., 0:2, :] + total[..., 2:4, :] + total[..., 4:6, :]
    hi, mid, low = three_parts(value)
    return jnp.concatenate([hi, mid, low, jnp.zeros_like(hi)], axis=-2)


def pair_kernel(a, b, o):
    o[:, :DATA, :] = (a[:, :DATA, :].astype(F32) + b[:, :DATA, :].astype(F32)).astype(BF16)
    o[:, DATA:, :] = resplit(a[:, DATA:, :].astype(F32) + b[:, DATA:, :].astype(F32)).astype(BF16)


def pair_add(a, b):
    spec = pl.BlockSpec((8, PIECE, 128), lambda i: (i, 0, 0))
    return pl.pallas_call(
        pair_kernel,
        grid=(PIECES // 8,),
        in_specs=[spec, spec],
        out_specs=spec,
        out_shape=jax.ShapeDtypeStruct((PIECES, PIECE, 128), BF16),
        interpret=INTERPRET,
        name="pair_add",
    )(a, b)


def sum_kernel(a, o, acc):
    i = pl.program_id(0)

    @pl.when(i == 0)
    def _():
        acc[...] = jnp.zeros_like(acc)

    acc[...] += jnp.sum(a[...].astype(F32), axis=0)

    @pl.when(i == pl.num_programs(0) - 1)
    def _():
        o[:DATA, :] = acc[:DATA, :].astype(BF16)
        o[DATA:, :] = resplit(acc[DATA:, :]).astype(BF16)


def chip_sum(a):
    return pl.pallas_call(
        sum_kernel,
        grid=(PIECES // 16,),
        in_specs=[pl.BlockSpec((16, PIECE, 128), lambda i: (i, 0, 0))],
        out_specs=pl.BlockSpec((PIECE, 128), lambda i: (0, 0)),
        out_shape=jax.ShapeDtypeStruct((PIECE, 128), BF16),
        scratch_shapes=[pltpu.VMEM((PIECE, 128), F32)],
        interpret=INTERPRET,
        name="chip_sum",
    )(a)


def finish_kernel(g0, g1, tail, dx, gin, gout, gtok, gbias, loss):
    last = tail[DATA:, :].astype(F32)
    last = last[0:1, :] + last[2:3, :] + last[4:5, :]
    total = last[0:1, 1:2]
    i = pl.program_id(0)

    @pl.when(i == 0)
    def _():
        loss[...] = jnp.broadcast_to(last[0:1, 0:1] / total, (8, 128))

    def piece(p, carry):
        rows = pl.ds(pl.multiple_of(p * 16, 16), 16)
        for j in range(2 * BLOCKS):
            g = (g0, g1)[j // BLOCKS]
            jj = j % BLOCKS
            value = (g[p, jj * 16 : (jj + 1) * 16, :].astype(F32) / total).astype(BF16)
            if j < 20:
                gin[rows, j * 128 : (j + 1) * 128] = value
            else:
                gout[rows, (j - 20) * 128 : (j - 19) * 128] = value
        return carry

    lax.fori_loop(0, 8, piece, 0)
    gtok[...] = (dx[...] / total).astype(BF16)
    e = g0[:, DATA:, :].astype(F32)
    gbias[...] = (e[:, 0:2, :] + e[:, 2:4, :] + e[:, 4:6, :]) / total


def finish(gathered, dx):
    return pl.pallas_call(
        finish_kernel,
        grid=(8,),
        in_specs=[
            pl.BlockSpec((8, None, PIECE, 128), lambda i: (i, 0, 0, 0)),
            pl.BlockSpec((8, None, PIECE, 128), lambda i: (i, 1, 0, 0)),
            pl.BlockSpec((None, None, PIECE, 128), lambda i: (10, 0, 0, 0)),
            pl.BlockSpec((64, D), lambda i: (i, 0)),
        ],
        out_specs=[
            pl.BlockSpec((128, COLS), lambda i: (i, 0)),
            pl.BlockSpec((128, D), lambda i: (i, 0)),
            pl.BlockSpec((64, D), lambda i: (i, 0)),
            pl.BlockSpec((8, 2, 128), lambda i: (i, 0, 0)),
            pl.BlockSpec((8, 128), lambda i: (0, 0)),
        ],
        out_shape=[
            jax.ShapeDtypeStruct((D, COLS), BF16),
            jax.ShapeDtypeStruct((D, D), BF16),
            jax.ShapeDtypeStruct((ROWS, D), BF16),
            jax.ShapeDtypeStruct((PIECES, 2, 128), F32),
            jax.ShapeDtypeStruct((8, 128), F32),
        ],
        interpret=INTERPRET,
        name="finish",
    )(gathered, gathered, gathered, dx)


def shards(tokens, labels, lengths, targets, w_in, b_in, w_out):
    core = lax.axis_index("c").astype(jnp.int32)
    meta = jnp.concatenate([lengths, core[None]])
    out, dx, mine, send = local_step(
        meta, targets.reshape(4, 128), tokens, labels, w_in, b_in.reshape(1, COLS), w_out
    )
    other = lax.ppermute(send, "c", [(0, 1), (1, 0)])
    both = pair_add(mine, other)
    spread = lax.all_to_all(both, CHIPS, 0, 0, tiled=True)
    piece = chip_sum(spread)
    gathered = lax.all_gather(piece, AXES, axis=0, tiled=False).reshape(PIECES, 2, PIECE, 128)
    gin, gout, gtok, gbias, loss = finish(gathered, dx)
    return out, loss[0, 0], gtok, gin, gbias[:10].reshape(COLS), gout


def solution(mesh):
    torus = Mesh(mesh.devices.reshape(4, 4, 4, 2), AXES)
    placed = (P(AXES, None), P(AXES, None), P(AXES), P(AXES), P(), P(), P())
    return jax.shard_map(
        shards,
        mesh=torus,
        in_specs=placed,
        out_specs=(P(AXES, None), P(), P(AXES, None), P(), P(), P()),
        check_vma=False,
    )
```

```python
import functools

import jax
import jax.numpy as jnp
from jax import lax
from jax.experimental import pallas as pl
from jax.experimental.pallas import tpu as pltpu
from jax.sharding import Mesh
from jax.sharding import PartitionSpec as P

D = 1024
HEADS = 4
VDIM = 256
QKDIM = 64
LMAX = 256
COLS = 2560
REST = 1536
ROWS = 512
QCOL = 1024
KCOL = 1280
AXES = ("z", "x", "y", "c")
CHIPS = ("z", "x", "y")
PIECES = 64
BLOCKS_A = 8
BLOCKS_B = 6
PIECE_A = BLOCKS_A * 16 + 8
PIECE_B = BLOCKS_B * 16 + 8
EPS = 1e-05
F32 = jnp.float32
BF16 = jnp.bfloat16
VM = pl.BlockSpec(memory_space=pltpu.VMEM)
SM = pl.BlockSpec(memory_space=pltpu.SMEM)
HBM = pl.BlockSpec(memory_space=pl.ANY)


def cost(flops):
    return pl.CostEstimate(flops=flops, transcendentals=0, bytes_accessed=8 * 2**20)


def sigmoid(h):
    return 0.5 * jnp.tanh(0.5 * h) + 0.5


def silu_slope(h, sg):
    return sg * (1.0 + h * (1.0 - sg))


def nn(a, b):
    return jnp.dot(a, b, preferred_element_type=F32)


def nt(a, b):
    return lax.dot_general(a, b, (((1,), (1,)), ((), ())), preferred_element_type=F32)


def tn(a, b):
    return lax.dot_general(a, b, (((0,), (0,)), ((), ())), preferred_element_type=F32)


def three_parts(value):
    hi = value.astype(BF16).astype(F32)
    rest = value - hi
    mid = rest.astype(BF16).astype(F32)
    low = (rest - mid).astype(BF16).astype(F32)
    return hi, mid, low


def row_stats(x):
    center = x - jnp.mean(x, axis=-1, keepdims=True)
    spread = jnp.mean(center * center, axis=-1, keepdims=True)
    return center, lax.rsqrt(spread + EPS)


def allowed_mask(length):
    i = lax.broadcasted_iota(jnp.int32, (LMAX, LMAX), 0)
    j = lax.broadcasted_iota(jnp.int32, (LMAX, LMAX), 1)
    return (j <= i) & (j < length)


def wide_row(ref, first, count):
    return jnp.concatenate([ref[j : j + 1, :] for j in range(first, first + count)], axis=1)


def pack(pay, blocks, j, value):
    half, jj = j // blocks, j % blocks
    pay[half, :, jj * 16 : (jj + 1) * 16, :] = value.astype(BF16).reshape(PIECES, 16, 128)


def forward_kernel(
    lens, tgt, tok, lab, win_hbm, bias, wout_hbm,
    out, mine, send, normed_t_out, acts_out, slope_out, dm_out, cot_out, dhu_out, bsum,
    win, wout, normed, normed_t, gate_h, gate_a, acts, slope, mixed, gated_t, dm, cot, dhu, lsum, csum, pay, sems,
):
    core = lax.axis_index("c")
    load_in = pltpu.make_async_copy(win_hbm, win, sems.at[0])
    load_out = pltpu.make_async_copy(wout_hbm, wout, sems.at[1])
    load_in.start()
    load_out.start()
    bsum[...] = jnp.zeros_like(bsum)
    lsum[...] = jnp.zeros_like(lsum)
    csum[...] = jnp.zeros_like(csum)
    lane = lax.broadcasted_iota(jnp.int32, (8, 128), 1)
    line = lax.broadcasted_iota(jnp.int32, (8, 128), 0)

    def prologue(r, carry):
        rows = pl.ds(pl.multiple_of(r * 128, 128), 128)
        length = lens[r // 2]
        place = (r % 2) * 128 + lax.broadcasted_iota(jnp.int32, (128, 128), 0)
        marks = jnp.transpose(jnp.broadcast_to(tgt[pl.ds(r, 1), :].astype(F32), (128, 128)))
        chosen = ((marks == 1.0) | (place == length - 1)) & (place < length)
        flag = jnp.where(chosen, 1.0, 0.0)
        csum[...] += jnp.sum(flag, axis=0, keepdims=True)
        wide = jnp.concatenate([flag] * 8, axis=1)
        cot[rows, :] = jnp.where(wide > 0.0, lab[rows, :].astype(F32), 0.0).astype(BF16)
        center, inv = row_stats(tok[rows, :].astype(F32))
        y = center * inv
        normed[rows, :] = y.astype(BF16)
        normed_t[:, rows] = jnp.transpose(y).astype(BF16)
        return carry

    lax.fori_loop(0, 4, prologue, 0)
    save_nt = pltpu.make_async_copy(normed_t, normed_t_out, sems.at[2])
    save_cot = pltpu.make_async_copy(cot, cot_out, sems.at[3])
    save_nt.start()
    save_cot.start()
    load_in.wait()

    for c in range(5):
        h = nn(normed[...], win[:, c * 512 : (c + 1) * 512]) + wide_row(bias, 4 * c, 4)
        sg = sigmoid(h)
        if c < 2:
            gate_h[:, c * 512 : (c + 1) * 512] = silu_slope(h, sg).astype(BF16)
            gate_a[:, c * 512 : (c + 1) * 512] = (h * sg).astype(BF16)
        else:
            slope[:, (c - 2) * 512 : (c - 1) * 512] = silu_slope(h, sg).astype(BF16)
            acts[:, (c - 2) * 512 : (c - 1) * 512] = (h * sg).astype(BF16)
    save_acts = pltpu.make_async_copy(acts, acts_out, sems.at[4])
    save_slope = pltpu.make_async_copy(slope, slope_out, sems.at[5])
    save_acts.start()
    save_slope.start()

    for n in range(2):
        rows = slice(n * LMAX, (n + 1) * LMAX)
        allowed = allowed_mask(lens[n])
        for h in range(HEADS):
            q = acts[rows, QCOL + h * QKDIM : QCOL + (h + 1) * QKDIM]
            k = acts[rows, KCOL + h * QKDIM : KCOL + (h + 1) * QKDIM]
            s = nt(q, k)
            w = jnp.where(allowed, s * sigmoid(s), 0.0).astype(BF16)
            mixed[rows, h * VDIM : (h + 1) * VDIM] = nn(w, acts[rows, h * VDIM : (h + 1) * VDIM])

    load_out.wait()

    def gate(r, carry):
        rows = pl.ds(pl.multiple_of(r * 128, 128), 128)
        center, inv = row_stats(mixed[rows, :])
        y = center * inv
        u = gate_a[rows, :].astype(F32)
        gated = (y * u).astype(BF16)
        gated_t[:, rows] = jnp.transpose(gated.astype(F32)).astype(BF16)
        length = lens[r // 2]
        place = (r % 2) * 128 + lax.broadcasted_iota(jnp.int32, (128, D), 0)
        full = tok[rows, :].astype(F32) + nn(gated, wout[...])
        rounded = jnp.where(place < length, full, 0.0).astype(BF16)
        out[rows, :] = rounded
        c = cot[rows, :]
        lsum[...] += jnp.sum(c.astype(F32) * rounded.astype(F32), axis=0, keepdims=True)
        dg = nt(c, wout[...]).astype(BF16).astype(F32)
        dy = dg * u
        du = (dg * y).astype(BF16).astype(F32)
        m1 = jnp.mean(dy, axis=-1, keepdims=True)
        m2 = jnp.mean(dy * y, axis=-1, keepdims=True)
        dm[rows, :] = (inv * (dy - m1 - y * m2)).astype(BF16)
        dh = du * gate_h[rows, :].astype(F32)
        dhu[rows, :] = dh.astype(BF16)
        bsum[0:1, :] += jnp.sum(dh, axis=0, keepdims=True)
        return carry

    lax.fori_loop(0, 4, gate, 0)
    save_dm = pltpu.make_async_copy(dm, dm_out, sems.at[6])
    save_dhu = pltpu.make_async_copy(dhu, dhu_out, sems.at[7])
    save_dm.start()
    save_dhu.start()

    for c in range(2):
        g = nn(gated_t[...], cot[:, c * 512 : (c + 1) * 512])
        for i in range(4):
            pack(pay, BLOCKS_A, 4 * c + i, g[:, i * 128 : (i + 1) * 128])
    for c in range(2):
        g = nn(normed_t[...], dhu[:, c * 512 : (c + 1) * 512])
        for i in range(4):
            pack(pay, BLOCKS_A, 8 + 4 * c + i, g[:, i * 128 : (i + 1) * 128])

    loss = jnp.sum(lsum[...], axis=1, keepdims=True)
    tail = jnp.where(lane == 0, jnp.broadcast_to(loss, (8, 128)), 0.0)
    tail = jnp.where(lane == 1, jnp.broadcast_to(csum[...], (8, 128)), tail)
    hi, mid, low = three_parts(tail)
    ext = jnp.where(line == 0, hi, jnp.where(line == 2, mid, jnp.where(line == 4, low, 0.0)))
    for half in range(2):
        pay[half, :, BLOCKS_A * 16 :, :] = jnp.zeros((PIECES, 8, 128), BF16)
        pay[half, 0, BLOCKS_A * 16 :, :] = ext.astype(BF16)

    to_send = pltpu.make_async_copy(pay.at[1 - core], send, sems.at[8])
    to_keep = pltpu.make_async_copy(pay.at[core], mine, sems.at[9])
    to_send.start()
    to_keep.start()
    for copy in (save_nt, save_cot, save_acts, save_slope, save_dm, save_dhu, to_send, to_keep):
        copy.wait()


def forward_step(lens, tgt, tok, lab, win, bias, wout):
    half = jax.ShapeDtypeStruct((PIECES, PIECE_A, 128), BF16)
    saved = [(D, ROWS), (ROWS, REST), (ROWS, REST), (ROWS, D), (ROWS, D), (ROWS, D)]
    return pl.pallas_call(
        forward_kernel,
        in_specs=[SM, VM, VM, VM, HBM, VM, HBM],
        out_specs=[VM] + [HBM] * 8 + [VM],
        out_shape=[jax.ShapeDtypeStruct((ROWS, D), BF16), half, half]
        + [jax.ShapeDtypeStruct(s, BF16) for s in saved]
        + [jax.ShapeDtypeStruct((1, D), F32)],
        scratch_shapes=[
            pltpu.VMEM((D, COLS), BF16),
            pltpu.VMEM((D, D), BF16),
            pltpu.VMEM((ROWS, D), BF16),
            pltpu.VMEM((D, ROWS), BF16),
            pltpu.VMEM((ROWS, D), BF16),
            pltpu.VMEM((ROWS, D), BF16),
            pltpu.VMEM((ROWS, REST), BF16),
            pltpu.VMEM((ROWS, REST), BF16),
            pltpu.VMEM((ROWS, D), F32),
            pltpu.VMEM((D, ROWS), BF16),
            pltpu.VMEM((ROWS, D), BF16),
            pltpu.VMEM((ROWS, D), BF16),
            pltpu.VMEM((ROWS, D), BF16),
            pltpu.VMEM((1, D), F32),
            pltpu.VMEM((1, 128), F32),
            pltpu.VMEM((2, PIECES, PIECE_A, 128), BF16),
            pltpu.SemaphoreType.DMA((10,)),
        ],
        compiler_params=pltpu.CompilerParams(vmem_limit_bytes=48 * 2**20),
        cost_estimate=cost(16 * 10**9),
        name="forward_step",
    )(lens, tgt, tok, lab, win, bias, wout)


def attention_kernel(lens, acts, slope, dm, dh, bsum, dqk):
    bsum[...] = jnp.zeros_like(bsum)
    for n in range(2):
        rows = slice(n * LMAX, (n + 1) * LMAX)
        allowed = allowed_mask(lens[n])
        for h in range(HEADS):
            q = acts[rows, QCOL + h * QKDIM : QCOL + (h + 1) * QKDIM]
            k = acts[rows, KCOL + h * QKDIM : KCOL + (h + 1) * QKDIM]
            vc = slice(h * VDIM, (h + 1) * VDIM)
            d = dm[rows, vc]
            s = nt(q, k)
            sg = sigmoid(s)
            w = jnp.where(allowed, s * sg, 0.0).astype(BF16)
            dw = nt(d, acts[rows, vc]).astype(BF16).astype(F32)
            dv = tn(w, d).astype(BF16).astype(F32)
            ds = jnp.where(allowed, dw * silu_slope(s, sg), 0.0).astype(BF16)
            dqk[rows, h * QKDIM : (h + 1) * QKDIM] = nn(ds, k)
            dqk[rows, 256 + h * QKDIM : 256 + (h + 1) * QKDIM] = tn(ds, q)
            dhv = dv * slope[rows, vc].astype(F32)
            dh[rows, vc] = dhv.astype(BF16)
            bsum[0:1, vc] += jnp.sum(dhv, axis=0, keepdims=True)
        dhq = dqk[rows, :].astype(BF16).astype(F32) * slope[rows, QCOL:].astype(F32)
        dh[rows, QCOL:] = dhq.astype(BF16)
        bsum[0:1, QCOL:] += jnp.sum(dhq, axis=0, keepdims=True)


def attention_back(lens, acts, slope, dm):
    return pl.pallas_call(
        attention_kernel,
        in_specs=[SM, VM, VM, VM],
        out_specs=[VM, VM],
        out_shape=[jax.ShapeDtypeStruct((ROWS, REST), BF16), jax.ShapeDtypeStruct((1, REST), F32)],
        scratch_shapes=[pltpu.VMEM((ROWS, 512), F32)],
        cost_estimate=cost(6 * 10**9),
        name="attention_back",
    )(lens, acts, slope, dm)


def weights_kernel(normed_t, dh, bsum_u, bsum_r, after, mine, send, pay, ext, sems):
    core = lax.axis_index("c")
    for c in range(3):
        g = nn(normed_t[...], dh[:, c * 512 : (c + 1) * 512])
        for i in range(4):
            pack(pay, BLOCKS_B, 4 * c + i, g[:, i * 128 : (i + 1) * 128])
    ext[...] = jnp.zeros_like(ext)
    for j in range(COLS // 128):
        row = bsum_u[0:1, j * 128 : (j + 1) * 128] if j < 8 else bsum_r[0:1, (j - 8) * 128 : (j - 7) * 128]
        parts = three_parts(row)
        base = 8 * (j // 2) + j % 2
        for t in range(3):
            ext[base + 2 * t : base + 2 * t + 1, :] = parts[t]
    for half in range(2):
        pay[half, :, BLOCKS_B * 16 :, :] = jnp.zeros((PIECES, 8, 128), BF16)
        for p in range(10):
            pay[half, p, BLOCKS_B * 16 :, :] = ext[8 * p : 8 * p + 8, :].astype(BF16)
    to_send = pltpu.make_async_copy(pay.at[1 - core], send, sems.at[0])
    to_keep = pltpu.make_async_copy(pay.at[core], mine, sems.at[1])
    to_send.start()
    to_keep.start()
    to_send.wait()
    to_keep.wait()


def weights_step(normed_t, dh, bsum_u, bsum_r, after):
    half = jax.ShapeDtypeStruct((PIECES, PIECE_B, 128), BF16)
    return pl.pallas_call(
        weights_kernel,
        in_specs=[VM, VM, VM, VM, HBM],
        out_specs=[HBM, HBM],
        out_shape=[half, half],
        scratch_shapes=[
            pltpu.VMEM((2, PIECES, PIECE_B, 128), BF16),
            pltpu.VMEM((80, 128), F32),
            pltpu.SemaphoreType.DMA((2,)),
        ],
        cost_estimate=cost(4 * 10**9),
        name="weights_step",
    )(normed_t, dh, bsum_u, bsum_r, after)


def rows_kernel(dhu, dhr, win, tok, cot, after, dx, acc):
    i = pl.program_id(0)

    @pl.when(i == 0)
    def _():
        acc[...] = nt(dhu[...], win[...])

    @pl.when((i > 0) & (i < 2))
    def _():
        acc[...] += nt(dhu[...], win[...])

    @pl.when(i >= 2)
    def _():
        acc[...] += nt(dhr[...], win[...])

    @pl.when(i == 4)
    def _():
        def back(r, carry):
            rows = pl.ds(pl.multiple_of(r * 128, 128), 128)
            dn = acc[rows, :].astype(BF16).astype(F32)
            center, inv = row_stats(tok[rows, :].astype(F32))
            y = center * inv
            m1 = jnp.mean(dn, axis=-1, keepdims=True)
            m2 = jnp.mean(dn * y, axis=-1, keepdims=True)
            dx[rows, :] = inv * (dn - m1 - y * m2) + cot[rows, :].astype(F32)
            return carry

        lax.fori_loop(0, 4, back, 0)


def rows_step(dhu, dhr, win, tok, cot, after):
    whole = pl.BlockSpec((ROWS, D), lambda i: (0, 0))
    return pl.pallas_call(
        rows_kernel,
        grid=(5,),
        in_specs=[
            pl.BlockSpec((ROWS, 512), lambda i: (0, jnp.minimum(i, 1))),
            pl.BlockSpec((ROWS, 512), lambda i: (0, jnp.maximum(i - 2, 0))),
            pl.BlockSpec((D, 512), lambda i: (0, i)),
            whole,
            whole,
            HBM,
        ],
        out_specs=whole,
        out_shape=jax.ShapeDtypeStruct((ROWS, D), F32),
        scratch_shapes=[pltpu.VMEM((ROWS, D), F32)],
        cost_estimate=cost(6 * 10**9),
        name="rows_step",
    )(dhu, dhr, win, tok, cot, after)


def resplit(total):
    value = total[..., 0:2, :] + total[..., 2:4, :] + total[..., 4:6, :]
    hi, mid, low = three_parts(value)
    return jnp.concatenate([hi, mid, low, jnp.zeros_like(hi)], axis=-2)


def pair_kernel(a, b, o):
    data = a.shape[1] - 8
    o[:, :data, :] = (a[:, :data, :].astype(F32) + b[:, :data, :].astype(F32)).astype(BF16)
    o[:, data:, :] = resplit(a[:, data:, :].astype(F32) + b[:, data:, :].astype(F32)).astype(BF16)


def pair_add(a, b):
    spec = pl.BlockSpec((16,) + a.shape[1:], lambda i: (i, 0, 0))
    return pl.pallas_call(
        pair_kernel,
        grid=(PIECES // 16,),
        in_specs=[spec, spec],
        out_specs=spec,
        out_shape=jax.ShapeDtypeStruct(a.shape, BF16),
        cost_estimate=cost(2 * 10**9),
        name="pair_add",
    )(a, b)


def sum_kernel(a, o, acc, piece, sem):
    i = pl.program_id(0)
    data = a.shape[1] - 8

    @pl.when(i == 0)
    def _():
        acc[...] = jnp.zeros_like(acc)

    acc[...] += jnp.sum(a[...].astype(F32), axis=0)

    @pl.when(i == pl.num_programs(0) - 1)
    def _():
        piece[:data, :] = acc[:data, :].astype(BF16)
        piece[data:, :] = resplit(acc[data:, :]).astype(BF16)
        copies = [pltpu.make_async_copy(piece, o.at[p], sem.at[p]) for p in range(PIECES)]
        for copy in copies:
            copy.start()
        for copy in copies:
            copy.wait()


def chip_sum(a):
    _, size, _ = a.shape
    return pl.pallas_call(
        sum_kernel,
        grid=(PIECES // 16,),
        in_specs=[pl.BlockSpec((16, size, 128), lambda i: (i, 0, 0))],
        out_specs=HBM,
        out_shape=jax.ShapeDtypeStruct(a.shape, BF16),
        scratch_shapes=[
            pltpu.VMEM((size, 128), F32),
            pltpu.VMEM((size, 128), BF16),
            pltpu.SemaphoreType.DMA((PIECES,)),
        ],
        cost_estimate=cost(2 * 10**9),
        name="chip_sum",
    )(a)


def finish_a_kernel(own, other, tail, dx, gin, gout, gtok, scale, loss):
    core = lax.axis_index("c")
    last = tail[BLOCKS_A * 16 :, :].astype(F32)
    last = last[0:1, :] + last[2:3, :] + last[4:5, :]
    inverse = 1.0 / last[0:1, 1:2]
    scale[...] = jnp.broadcast_to(inverse, (8, 128))
    loss[...] = last[0:1, 0:1] * inverse

    def move(src, dst):
        def piece(p, carry):
            rows = pl.ds(pl.multiple_of(p * 16, 16), 16)
            for j in range(BLOCKS_A):
                value = src[p, j * 16 : (j + 1) * 16, :].astype(F32) * inverse
                dst[rows, j * 128 : (j + 1) * 128] = value.astype(BF16)
            return carry

        lax.fori_loop(0, 16, piece, 0)

    @pl.when(core == 0)
    def _():
        move(own, gout)
        move(other, gin)

    @pl.when(core == 1)
    def _():
        move(other, gout)
        move(own, gin)

    gtok[...] = (dx[...] * inverse).astype(BF16)


def finish_a(own, other, dx):
    spec = pl.BlockSpec((16, PIECE_A, 128), lambda i: (i, 0, 0))
    return pl.pallas_call(
        finish_a_kernel,
        grid=(4,),
        in_specs=[spec, spec, pl.BlockSpec((None, PIECE_A, 128), lambda i: (0, 0, 0)), pl.BlockSpec((128, D), lambda i: (i, 0))],
        out_specs=[
            pl.BlockSpec((256, D), lambda i: (i, 0)),
            pl.BlockSpec((256, D), lambda i: (i, 0)),
            pl.BlockSpec((128, D), lambda i: (i, 0)),
            pl.BlockSpec((8, 128), lambda i: (0, 0)),
            pl.BlockSpec((1, 1), lambda i: (0, 0)),
        ],
        out_shape=[
            jax.ShapeDtypeStruct((D, COLS), BF16),
            jax.ShapeDtypeStruct((D, D), BF16),
            jax.ShapeDtypeStruct((ROWS, D), BF16),
            jax.ShapeDtypeStruct((8, 128), F32),
            jax.ShapeDtypeStruct((1, 1), F32),
        ],
        cost_estimate=cost(3 * 10**9),
        name="finish_a",
    )(own, other, own, dx)


def finish_b_kernel(own, other, tail, scale, gin_in, gin, gbias, buf, sems):
    core = lax.axis_index("c")
    i = pl.program_id(0)
    inverse = scale[0:1, 0:1]

    def move(src, first):
        def piece(p, carry):
            rows = pl.ds(pl.multiple_of(p * 16, 16), 16)
            for j in range(BLOCKS_B):
                value = src[p, j * 16 : (j + 1) * 16, :].astype(F32) * inverse
                buf[i, rows, (first + j) * 128 : (first + j + 1) * 128] = value.astype(BF16)
            return carry

        lax.fori_loop(0, 16, piece, 0)

    @pl.when(core == 0)
    def _():
        move(own, 0)
        move(other, BLOCKS_B)

    @pl.when(core == 1)
    def _():
        move(other, 0)
        move(own, BLOCKS_B)

    def save(t):
        return pltpu.make_async_copy(buf.at[t], gin.at[pl.ds(t * 256, 256), pl.ds(D, REST)], sems.at[t])

    save(i).start()

    @pl.when(i == 0)
    def _():
        for p in range(10):
            e = tail[p, BLOCKS_B * 16 :, :].astype(F32)
            gbias[2 * p : 2 * p + 2, :] = (e[0:2, :] + e[2:4, :] + e[4:6, :]) * inverse

    @pl.when(i == 3)
    def _():
        for t in range(4):
            save(t).wait()


def finish_b(own, other, scale, gin):
    spec = pl.BlockSpec((16, PIECE_B, 128), lambda i: (i, 0, 0))
    return pl.pallas_call(
        finish_b_kernel,
        grid=(4,),
        in_specs=[
            spec,
            spec,
            pl.BlockSpec((16, PIECE_B, 128), lambda i: (0, 0, 0)),
            pl.BlockSpec((8, 128), lambda i: (0, 0)),
            HBM,
        ],
        out_specs=[HBM, pl.BlockSpec((20, 128), lambda i: (0, 0))],
        out_shape=[jax.ShapeDtypeStruct((D, COLS), BF16), jax.ShapeDtypeStruct((20, 128), F32)],
        input_output_aliases={4: 0},
        scratch_shapes=[pltpu.VMEM((4, 256, REST), BF16), pltpu.SemaphoreType.DMA((4,))],
        cost_estimate=cost(3 * 10**9),
        name="finish_b",
    )(own, other, own, scale, gin)


def swap(value):
    return lax.ppermute(value, "c", [(0, 1), (1, 0)])


def exchange(value):
    return lax.all_to_all(value, CHIPS, 0, 0, tiled=True)


def shards(tokens, labels, lengths, targets, w_in, b_in, w_out):
    out, mine_a, send_a, normed_t, acts, slope, dm, cot, dhu, bsum_u = forward_step(
        lengths, targets.reshape(4, 128), tokens, labels, w_in, b_in.reshape(20, 128), w_out
    )
    other_a = swap(send_a)
    dhr, bsum_r = attention_back(lengths, acts, slope, dm)
    pair_a = pair_add(mine_a, other_a)
    spread_a = exchange(pair_a)
    mine_b, send_b = weights_step(normed_t, dhr, bsum_u, bsum_r, pair_a)
    other_b = swap(send_b)
    dx = rows_step(dhu, dhr, w_in, tokens, cot, mine_b)
    pair_b = pair_add(mine_b, other_b)
    spread_b = exchange(pair_b)
    copies_a = chip_sum(spread_a)
    own_a = exchange(copies_a)
    copies_b = chip_sum(spread_b)
    own_b = exchange(copies_b)
    gin, gout, gtok, scale, loss = finish_a(own_a, swap(own_a), dx)
    gin, gbias = finish_b(own_b, swap(own_b), scale, gin)
    return out, loss.reshape(()), gtok, gin, gbias.reshape(COLS), gout


def solution(mesh):
    torus = Mesh(mesh.devices.reshape(4, 4, 4, 2), AXES)
    placed = (P(AXES, None), P(AXES, None), P(AXES), P(AXES), P(), P(), P())
    return jax.shard_map(
        shards,
        mesh=torus,
        in_specs=placed,
        out_specs=(P(AXES, None), P(), P(AXES, None), P(), P(), P()),
        check_vma=False,
    )
```

```python
import functools

import jax
import jax.numpy as jnp
from jax import lax
from jax.experimental import pallas as pl
from jax.experimental.pallas import tpu as pltpu
from jax.sharding import Mesh
from jax.sharding import PartitionSpec as P

D = 1024
HEADS = 4
VDIM = 256
QKDIM = 64
LMAX = 256
COLS = 2560
REST = 1536
ROWS = 512
QCOL = 1024
KCOL = 1280
AXES = ("z", "x", "y", "c")
CHIPS = ("z", "x", "y")
PLANES = (("x", "y"), ("z", "y"), ("z", "x"))
PIECES = 64
BLOCKS = 14
COLORS = 3
DEEP = 80
EXTRA = 64
GROUP = 16
EPS = 1e-05
F32 = jnp.float32
BF16 = jnp.bfloat16
VM = pl.BlockSpec(memory_space=pltpu.VMEM)
SM = pl.BlockSpec(memory_space=pltpu.SMEM)
HBM = pl.BlockSpec(memory_space=pltpu.HBM)
ANY = pl.BlockSpec(memory_space=pl.ANY)


def cost(flops):
    return pl.CostEstimate(flops=flops, transcendentals=0, bytes_accessed=8 * 2**20)


def sigmoid(h):
    return 0.5 * jnp.tanh(0.5 * h) + 0.5


def silu_slope(h, sg):
    return sg * (1.0 + h * (1.0 - sg))


def nn(a, b):
    return jnp.dot(a, b, preferred_element_type=F32)


def nt(a, b):
    return lax.dot_general(a, b, (((1,), (1,)), ((), ())), preferred_element_type=F32)


def tn(a, b):
    return lax.dot_general(a, b, (((0,), (0,)), ((), ())), preferred_element_type=F32)


def three_parts(value):
    hi = value.astype(BF16).astype(F32)
    rest = value - hi
    mid = rest.astype(BF16).astype(F32)
    low = (rest - mid).astype(BF16).astype(F32)
    return hi, mid, low


def row_stats(x):
    center = x - jnp.mean(x, axis=-1, keepdims=True)
    spread = jnp.mean(center * center, axis=-1, keepdims=True)
    return center, lax.rsqrt(spread + EPS)


def allowed_mask(length):
    i = lax.broadcasted_iota(jnp.int32, (LMAX, LMAX), 0)
    j = lax.broadcasted_iota(jnp.int32, (LMAX, LMAX), 1)
    return (j <= i) & (j < length)


def wide_row(ref, first, count):
    return jnp.concatenate([ref[j : j + 1, :] for j in range(first, first + count)], axis=1)


def pack(pay, j, value):
    half, jj = j // BLOCKS, j % BLOCKS
    color, row = jj // 5, (jj % 5) * 16
    pay[half, color, :, row : row + 16, :] = value.astype(BF16).reshape(PIECES, 16, 128)


def local_kernel(
    lens_hbm, tgt_hbm, tok_hbm, lab_hbm, win_hbm, bias_hbm, wout_hbm,
    out_hbm, dx_hbm, mine, send,
    lens, tgt, tok, lab, win, bias, wout, out, dx,
    normed, normed_t, slope, acts, dh, mixed, gated_t, dm, wt, ws, cot, dqk, bsum, lsum, csum, ext, pay, sems,
):
    core = lax.axis_index("c")
    pairs = (
        (lens_hbm, lens), (tgt_hbm, tgt), (tok_hbm, tok), (lab_hbm, lab),
        (win_hbm, win), (bias_hbm, bias), (wout_hbm, wout),
    )
    loads = [pltpu.make_async_copy(a, b, sems.at[n]) for n, (a, b) in enumerate(pairs)]
    for load in loads:
        load.start()
    bsum[...] = jnp.zeros_like(bsum)
    lsum[...] = jnp.zeros_like(lsum)
    csum[...] = jnp.zeros_like(csum)
    ext[...] = jnp.zeros_like(ext)
    for load in loads[:4]:
        load.wait()

    def prologue(r, carry):
        rows = pl.ds(pl.multiple_of(r * 128, 128), 128)
        length = lens[r // 2]
        place = (r % 2) * 128 + lax.broadcasted_iota(jnp.int32, (128, 128), 0)
        marks = jnp.transpose(jnp.broadcast_to(tgt[pl.ds(r, 1), :].astype(F32), (128, 128)))
        chosen = ((marks == 1.0) | (place == length - 1)) & (place < length)
        flag = jnp.where(chosen, 1.0, 0.0)
        csum[...] += jnp.sum(flag, axis=0, keepdims=True)
        wide = jnp.concatenate([flag] * 8, axis=1)
        cot[rows, :] = jnp.where(wide > 0.0, lab[rows, :].astype(F32), 0.0).astype(BF16)
        center, inv = row_stats(tok[rows, :].astype(F32))
        y = center * inv
        normed[rows, :] = y.astype(BF16)
        normed_t[:, rows] = jnp.transpose(y).astype(BF16)
        return carry

    lax.fori_loop(0, 4, prologue, 0)
    loads[4].wait()
    loads[5].wait()

    for c in range(5):
        cols = slice(c * 512, (c + 1) * 512)
        h = nn(normed[...], win[:, cols]) + wide_row(bias, 4 * c, 4)
        sg = sigmoid(h)
        slope[:, cols] = silu_slope(h, sg).astype(BF16)
        acts[:, cols] = (h * sg).astype(BF16)

    for n in range(2):
        rows = slice(n * LMAX, (n + 1) * LMAX)
        allowed = allowed_mask(lens[n])
        for h in range(HEADS):
            q = acts[rows, D + QCOL + h * QKDIM : D + QCOL + (h + 1) * QKDIM]
            k = acts[rows, D + KCOL + h * QKDIM : D + KCOL + (h + 1) * QKDIM]
            s = nt(q, k)
            sg = sigmoid(s)
            w = jnp.where(allowed, s * sg, 0.0).astype(BF16)
            wt[n * HEADS + h] = w
            ws[n * HEADS + h] = jnp.where(allowed, silu_slope(s, sg), 0.0)
            mixed[rows, h * VDIM : (h + 1) * VDIM] = nn(w, acts[rows, D + h * VDIM : D + (h + 1) * VDIM])

    loads[6].wait()

    def gate(r, carry):
        rows = pl.ds(pl.multiple_of(r * 128, 128), 128)
        center, inv = row_stats(mixed[rows, :])
        y = center * inv
        u = acts[rows, :D].astype(F32)
        gated = (y * u).astype(BF16)
        gated_t[:, rows] = jnp.transpose(gated.astype(F32)).astype(BF16)
        length = lens[r // 2]
        place = (r % 2) * 128 + lax.broadcasted_iota(jnp.int32, (128, D), 0)
        full = tok[rows, :].astype(F32) + nn(gated, wout[...])
        rounded = jnp.where(place < length, full, 0.0).astype(BF16)
        out[rows, :] = rounded
        c = cot[rows, :]
        lsum[...] += jnp.sum(c.astype(F32) * rounded.astype(F32), axis=0, keepdims=True)
        dg = nt(c, wout[...]).astype(BF16).astype(F32)
        dy = dg * u
        du = (dg * y).astype(BF16).astype(F32)
        m1 = jnp.mean(dy, axis=-1, keepdims=True)
        m2 = jnp.mean(dy * y, axis=-1, keepdims=True)
        dm[rows, :] = (inv * (dy - m1 - y * m2)).astype(BF16)
        dhu = du * slope[rows, :D].astype(F32)
        dh[rows, :D] = dhu.astype(BF16)
        bsum[0:1, :D] += jnp.sum(dhu, axis=0, keepdims=True)
        return carry

    lax.fori_loop(0, 4, gate, 0)
    save_out = pltpu.make_async_copy(out, out_hbm, sems.at[7])
    save_out.start()

    for c in range(2):
        g = nn(gated_t[...], cot[:, c * 512 : (c + 1) * 512])
        for i in range(4):
            pack(pay, 20 + 4 * c + i, g[:, i * 128 : (i + 1) * 128])

    for n in range(2):
        rows = slice(n * LMAX, (n + 1) * LMAX)
        for h in range(HEADS):
            q = acts[rows, D + QCOL + h * QKDIM : D + QCOL + (h + 1) * QKDIM]
            k = acts[rows, D + KCOL + h * QKDIM : D + KCOL + (h + 1) * QKDIM]
            vc = slice(D + h * VDIM, D + (h + 1) * VDIM)
            d = dm[rows, h * VDIM : (h + 1) * VDIM]
            dw = nt(d, acts[rows, vc]).astype(BF16).astype(F32)
            dv = tn(wt[n * HEADS + h], d).astype(BF16).astype(F32)
            ds = (dw * ws[n * HEADS + h]).astype(BF16)
            dqk[rows, h * QKDIM : (h + 1) * QKDIM] = nn(ds, k)
            dqk[rows, 256 + h * QKDIM : 256 + (h + 1) * QKDIM] = tn(ds, q)
            dhv = dv * slope[rows, vc].astype(F32)
            dh[rows, vc] = dhv.astype(BF16)
            bsum[0:1, vc] += jnp.sum(dhv, axis=0, keepdims=True)
        dhq = dqk[rows, :].astype(BF16).astype(F32) * slope[rows, 2 * D :].astype(F32)
        dh[rows, 2 * D :] = dhq.astype(BF16)
        bsum[0:1, 2 * D :] += jnp.sum(dhq, axis=0, keepdims=True)

    for c in range(5):
        g = nn(normed_t[...], dh[:, c * 512 : (c + 1) * 512])
        for i in range(4):
            pack(pay, 4 * c + i, g[:, i * 128 : (i + 1) * 128])

    for j in range(COLS // 128):
        parts = three_parts(bsum[0:1, j * 128 : (j + 1) * 128])
        base = 8 * (j // 2) + j % 2
        for t in range(3):
            ext[base + 2 * t : base + 2 * t + 1, :] = parts[t]
    loss = jnp.sum(lsum[...], axis=1, keepdims=True)
    lane = lax.broadcasted_iota(jnp.int32, (1, 128), 1)
    tail = jnp.where(lane == 0, jnp.broadcast_to(loss, (1, 128)), jnp.where(lane == 1, csum[...], 0.0))
    parts = three_parts(tail)
    for t in range(3):
        ext[80 + 2 * t : 81 + 2 * t, :] = parts[t]
    for half in range(2):
        pay[half, 2, :, EXTRA:, :] = jnp.zeros((PIECES, 16, 128), BF16)
        for p in range(11):
            pay[half, 2, p, EXTRA : EXTRA + 8, :] = ext[8 * p : 8 * p + 8, :].astype(BF16)

    to_send = pltpu.make_async_copy(pay.at[1 - core], send, sems.at[8])
    to_keep = pltpu.make_async_copy(pay.at[core], mine, sems.at[9])
    to_send.start()
    to_keep.start()

    def back(r, carry):
        rows = pl.ds(pl.multiple_of(r * 128, 128), 128)
        dn = nt(dh[rows, :], win[...]).astype(BF16).astype(F32)
        center, inv = row_stats(tok[rows, :].astype(F32))
        y = center * inv
        m1 = jnp.mean(dn, axis=-1, keepdims=True)
        m2 = jnp.mean(dn * y, axis=-1, keepdims=True)
        dx[rows, :] = inv * (dn - m1 - y * m2) + cot[rows, :].astype(F32)
        return carry

    lax.fori_loop(0, 4, back, 0)
    save_dx = pltpu.make_async_copy(dx, dx_hbm, sems.at[10])
    save_dx.start()
    for copy in (save_out, to_send, to_keep, save_dx):
        copy.wait()


def local_step(lens, tgt, tok, lab, win, bias, wout):
    half = jax.ShapeDtypeStruct((COLORS, PIECES, DEEP, 128), BF16)
    wide = pltpu.VMEM((ROWS, COLS), BF16)
    rows = pltpu.VMEM((ROWS, D), BF16)
    turned = pltpu.VMEM((D, ROWS), BF16)
    return pl.pallas_call(
        local_kernel,
        in_specs=[HBM] * 7,
        out_specs=[HBM, HBM, HBM, HBM],
        out_shape=[jax.ShapeDtypeStruct((ROWS, D), BF16), jax.ShapeDtypeStruct((ROWS, D), F32), half, half],
        scratch_shapes=[
            pltpu.SMEM((2,), jnp.int32),
            pltpu.VMEM((4, 128), jnp.int32),
            rows,
            rows,
            pltpu.VMEM((D, COLS), BF16),
            pltpu.VMEM((20, 128), F32),
            pltpu.VMEM((D, D), BF16),
            rows,
            pltpu.VMEM((ROWS, D), F32),
            rows,
            turned,
            wide,
            wide,
            wide,
            pltpu.VMEM((ROWS, D), F32),
            turned,
            rows,
            pltpu.VMEM((2 * HEADS, LMAX, LMAX), BF16),
            pltpu.VMEM((2 * HEADS, LMAX, LMAX), F32),
            rows,
            pltpu.VMEM((ROWS, 512), F32),
            pltpu.VMEM((8, COLS), F32),
            pltpu.VMEM((1, D), F32),
            pltpu.VMEM((1, 128), F32),
            pltpu.VMEM((88, 128), F32),
            pltpu.VMEM((2, COLORS, PIECES, DEEP, 128), BF16),
            pltpu.SemaphoreType.DMA((11,)),
        ],
        compiler_params=pltpu.CompilerParams(vmem_limit_bytes=52 * 2**20),
        name="local_step",
    )(lens, tgt, tok, lab, win, bias, wout)


def resplit(total):
    value = total[..., 0:2, :] + total[..., 2:4, :] + total[..., 4:6, :]
    hi, mid, low = three_parts(value)
    return jnp.concatenate([hi, mid, low, jnp.zeros_like(hi)], axis=-2)


def put_sum(dst, total, extras):
    if extras:
        dst[:, :EXTRA, :] = total[:, :EXTRA, :].astype(BF16)
        dst[:, EXTRA : EXTRA + 8, :] = resplit(total[:, EXTRA : EXTRA + 8, :]).astype(BF16)
        dst[:, EXTRA + 8 :, :] = total[:, EXTRA + 8 :, :].astype(BF16)
    else:
        dst[...] = total.astype(BF16)


def places():
    return [lax.axis_index(a) for a in CHIPS]


ORDER = [(c, d) for d in (2, 1, 3, 0) for c in range(COLORS)]


def pair_kernel(a_hbm, b_hbm, *rest):
    outs, (a, b, o, sems) = rest[:12], rest[12:]
    spot = places()

    def load(n):
        c, d = ORDER[n]
        k = pl.ds(lax.rem(spot[c] + d, 4) * GROUP, GROUP)
        return (
            pltpu.make_async_copy(a_hbm.at[c, k], a.at[n], sems.at[0, n]),
            pltpu.make_async_copy(b_hbm.at[c, k], b.at[n], sems.at[1, n]),
        )

    for n in range(12):
        for copy in load(n):
            copy.start()
    saves = []
    for n in range(12):
        for copy in load(n):
            copy.wait()
        put_sum(o.at[n], a[n].astype(F32) + b[n].astype(F32), ORDER[n][0] == 2)
        saves.append(pltpu.make_async_copy(o.at[n], outs[n], sems.at[2, n]))
        saves[-1].start()
    for save in saves:
        save.wait()


CHUNK = (GROUP, DEEP, 128)


def pair_add(a, b):
    outs = pl.pallas_call(
        pair_kernel,
        in_specs=[ANY, ANY],
        out_specs=[ANY] * 12,
        out_shape=[jax.ShapeDtypeStruct(CHUNK, BF16)] * 12,
        scratch_shapes=[pltpu.VMEM((12,) + CHUNK, BF16)] * 3 + [pltpu.SemaphoreType.DMA((3, 12))],
        name="pair_add",
    )(a, b)
    return dict(zip(ORDER, outs))


def ring_sum_kernel(*rest):
    ins, outs, (buf, o, sems) = rest[:12], rest[12:15], rest[15:]
    for n in range(12):
        pltpu.make_async_copy(ins[n], buf.at[n], sems.at[n]).start()
    saves = []
    for c in range(COLORS):
        for d in range(4):
            n = 4 * c + d
            pltpu.make_async_copy(ins[n], buf.at[n], sems.at[n]).wait()
        total = sum(buf[4 * c + d].astype(F32) for d in range(4))
        put_sum(o.at[c], total, c == 2)
        saves.append(pltpu.make_async_copy(o.at[c], outs[c], sems.at[12 + c]))
        saves[-1].start()
    for save in saves:
        save.wait()


def ring_sum(chunks):
    return pl.pallas_call(
        ring_sum_kernel,
        in_specs=[ANY] * 12,
        out_specs=[ANY] * 3,
        out_shape=[jax.ShapeDtypeStruct(CHUNK, BF16)] * 3,
        scratch_shapes=[
            pltpu.VMEM((12,) + CHUNK, BF16),
            pltpu.VMEM((3,) + CHUNK, BF16),
            pltpu.SemaphoreType.DMA((15,)),
        ],
        name="ring_sum",
    )(*chunks)


def plane_sum_kernel(extras, a, o):
    total = jnp.sum(a[...].astype(F32), axis=0, keepdims=True)
    put_sum(o.at[0:1], total, extras)
    for p in range(1, GROUP):
        o[p] = o[0]


def plane_sum(a, extras):
    return pl.pallas_call(
        functools.partial(plane_sum_kernel, extras),
        in_specs=[VM],
        out_specs=VM,
        out_shape=jax.ShapeDtypeStruct(CHUNK, BF16),
        name="plane_sum",
    )(a)


def targets_of(half, color):
    blocks = [half * BLOCKS + jj for jj in range(BLOCKS) if jj // 5 == color]
    low = [j for j in blocks if j < 20]
    high = [j - 20 for j in blocks if j >= 20]
    return low, high


def finish_kernel(*rest):
    ins, dx_hbm = rest[:24], rest[24]
    gin, gout, gtok_hbm, gbias, loss = rest[25:30]
    buf, dx, gtok, vin, vout, sems, outs = rest[30:]
    core = lax.axis_index("c")
    spot = places()
    order = [(s, c, d) for s in range(2) for c in (2, 0, 1) for d in range(4)]

    def load(n):
        s, c, d = order[n]
        return pltpu.make_async_copy(ins[12 * s + 4 * c + d], buf.at[n], sems.at[n])

    load_dx = pltpu.make_async_copy(dx_hbm, dx, sems.at[24])
    for n in range(24):
        load(n).start()
    load_dx.start()
    for n in range(4):
        load(n).wait()
    last = buf[spot[2], 10, EXTRA : EXTRA + 8, :].astype(F32)
    last = last[0:1, :] + last[2:3, :] + last[4:5, :]
    inverse = 1.0 / last[0:1, 1:2]
    loss[...] = last[0:1, 0:1] * inverse
    for p in range(10):
        e = buf[spot[2], p, EXTRA : EXTRA + 8, :].astype(F32)
        gbias[2 * p : 2 * p + 2, :] = (e[0:2, :] + e[2:4, :] + e[4:6, :]) * inverse

    def unpack(half, n):
        _, c, d = order[n]
        base = pl.multiple_of(lax.rem(spot[c] + 4 - d, 4) * 256, 256)
        low, high = targets_of(half, c)
        dests = [(vin, j) for j in low] + [(vout, j) for j in high]

        def piece(q, carry):
            rows = pl.ds(pl.multiple_of(base + q * 16, 16), 16)
            for i, (ref, j) in enumerate(dests):
                value = buf[n, q, i * 16 : (i + 1) * 16, :].astype(F32) * inverse
                ref[rows, j * 128 : (j + 1) * 128] = value.astype(BF16)
            return carry

        lax.fori_loop(0, GROUP, piece, 0)
        copies = []
        for ref, dst, blocks, k in ((vin, gin, low, 0), (vout, gout, high, 1)):
            if blocks:
                window = (pl.ds(base, 256), pl.ds(blocks[0] * 128, len(blocks) * 128))
                copies.append(pltpu.make_async_copy(ref.at[window], dst.at[window], outs.at[k, n]))
        return copies

    def run(me):
        saves = []
        for n in range(24):
            if n >= 4:
                load(n).wait()
            copies = unpack(me if order[n][0] == 0 else 1 - me, n)
            for copy in copies:
                copy.start()
            saves += copies
        for save in saves:
            save.wait()

    @pl.when(core == 0)
    def _():
        run(0)

    @pl.when(core == 1)
    def _():
        run(1)

    load_dx.wait()
    gtok[...] = (dx[...] * inverse).astype(BF16)
    save = pltpu.make_async_copy(gtok, gtok_hbm, sems.at[25])
    save.start()
    save.wait()


def finish(chunks, dx):
    return pl.pallas_call(
        finish_kernel,
        in_specs=[ANY] * 24 + [HBM],
        out_specs=[HBM, HBM, HBM, VM, VM],
        out_shape=[
            jax.ShapeDtypeStruct((D, COLS), BF16),
            jax.ShapeDtypeStruct((D, D), BF16),
            jax.ShapeDtypeStruct((ROWS, D), BF16),
            jax.ShapeDtypeStruct((20, 128), F32),
            jax.ShapeDtypeStruct((1, 1), F32),
        ],
        scratch_shapes=[
            pltpu.VMEM((24,) + CHUNK, BF16),
            pltpu.VMEM((ROWS, D), F32),
            pltpu.VMEM((ROWS, D), BF16),
            pltpu.VMEM((D, COLS), BF16),
            pltpu.VMEM((D, D), BF16),
            pltpu.SemaphoreType.DMA((26,)),
            pltpu.SemaphoreType.DMA((2, 24)),
        ],
        compiler_params=pltpu.CompilerParams(vmem_limit_bytes=40 * 2**20),
        name="finish",
    )(*chunks, dx)


def swap(value):
    return lax.ppermute(value, "c", [(0, 1), (1, 0)])


def shift(value, color, d):
    return lax.ppermute(value, CHIPS[color], [(i, (i + d) % 4) for i in range(4)])


def exchange(value, color):
    return lax.all_to_all(value, PLANES[color], 0, 0, tiled=True)


def shards(tokens, labels, lengths, targets, w_in, b_in, w_out):
    out, dx, mine, send = local_step(
        lengths, targets.reshape(4, 128), tokens, labels, w_in, b_in.reshape(20, 128), w_out
    )
    chunks = pair_add(mine, swap(send))
    for c, d in ORDER:
        if d:
            chunks[c, d] = shift(chunks[c, d], c, d)
    partial = ring_sum([chunks[c, d] for c in range(COLORS) for d in range(4)])
    own = {}
    for c in range(COLORS):
        own[c, 0] = exchange(plane_sum(exchange(partial[c], c), c == 2), c)
    for d in (2, 1, 3):
        for c in range(COLORS):
            own[c, d] = shift(own[c, 0], c, d)
    keys = [(c, d) for c in range(COLORS) for d in range(4)]
    other = {key: swap(own[key]) for key in keys}
    gin, gout, gtok, gbias, loss = finish([own[k] for k in keys] + [other[k] for k in keys], dx)
    return out, loss.reshape(()), gtok, gin, gbias.reshape(COLS), gout


def solution(mesh):
    torus = Mesh(mesh.devices.reshape(4, 4, 4, 2), AXES)
    placed = (P(AXES, None), P(AXES, None), P(AXES), P(AXES), P(), P(), P())
    return jax.shard_map(
        shards,
        mesh=torus,
        in_specs=placed,
        out_specs=(P(AXES, None), P(), P(AXES, None), P(), P(), P()),
        check_vma=False,
    )
```

```python
import functools

import jax
import jax.numpy as jnp
from jax import lax
from jax.experimental import pallas as pl
from jax.experimental.pallas import tpu as pltpu
from jax.sharding import Mesh
from jax.sharding import PartitionSpec as P

D = 1024
HEADS = 4
VDIM = 256
QKDIM = 64
LMAX = 256
COLS = 2560
REST = 1536
ROWS = 512
QCOL = 1024
KCOL = 1280
AXES = ("z", "x", "y", "c")
CHIPS = ("z", "x", "y")
TURNS = ((0, 1, 2), (1, 2, 0), (2, 0, 1))
SHIFTS = (1, 3, 2)
PIECES = 64
BLOCKS = 14
COLORS = 3
DEEP = 80
EXTRA = 64
GROUP = 16
EPS = 1e-05
F32 = jnp.float32
BF16 = jnp.bfloat16
VM = pl.BlockSpec(memory_space=pltpu.VMEM)
SM = pl.BlockSpec(memory_space=pltpu.SMEM)
HBM = pl.BlockSpec(memory_space=pltpu.HBM)
ANY = pl.BlockSpec(memory_space=pl.ANY)


def cost(flops):
    return pl.CostEstimate(flops=flops, transcendentals=0, bytes_accessed=8 * 2**20)


def sigmoid(h):
    return 0.5 * jnp.tanh(0.5 * h) + 0.5


def silu_slope(h, sg):
    return sg * (1.0 + h * (1.0 - sg))


def nn(a, b):
    return jnp.dot(a, b, preferred_element_type=F32)


def nt(a, b):
    return lax.dot_general(a, b, (((1,), (1,)), ((), ())), preferred_element_type=F32)


def tn(a, b):
    return lax.dot_general(a, b, (((0,), (0,)), ((), ())), preferred_element_type=F32)


def three_parts(value):
    hi = value.astype(BF16).astype(F32)
    rest = value - hi
    mid = rest.astype(BF16).astype(F32)
    low = (rest - mid).astype(BF16).astype(F32)
    return hi, mid, low


def row_stats(x):
    center = x - jnp.mean(x, axis=-1, keepdims=True)
    spread = jnp.mean(center * center, axis=-1, keepdims=True)
    return center, lax.rsqrt(spread + EPS)


def allowed_mask(length):
    i = lax.broadcasted_iota(jnp.int32, (LMAX, LMAX), 0)
    j = lax.broadcasted_iota(jnp.int32, (LMAX, LMAX), 1)
    return (j <= i) & (j < length)


def wide_row(ref, first, count):
    return jnp.concatenate([ref[j : j + 1, :] for j in range(first, first + count)], axis=1)


def pack(pay, j, value):
    half, jj = j // BLOCKS, j % BLOCKS
    color, row = jj // 5, (jj % 5) * 16
    pay[half, color, :, row : row + 16, :] = value.astype(BF16).reshape(PIECES, 16, 128)


def local_kernel(
    lens_hbm, tgt_hbm, tok_hbm, lab_hbm, win_hbm, bias_hbm, wout_hbm,
    out_hbm, dx_hbm, mine_0, mine_1, mine_2, send_0, send_1, send_2,
    lens, tgt, tok, lab, win, bias, wout, out, dx,
    normed, normed_t, slope, acts, dh, mixed, gated_t, dm, wt, ws, cot, dqk, bsum, lsum, csum, ext, pay, sems,
):
    core = lax.axis_index("c")
    pairs = (
        (lens_hbm, lens), (tgt_hbm, tgt), (tok_hbm, tok), (lab_hbm, lab),
        (win_hbm, win), (bias_hbm, bias), (wout_hbm, wout),
    )
    loads = [pltpu.make_async_copy(a, b, sems.at[n]) for n, (a, b) in enumerate(pairs)]
    for load in loads:
        load.start()
    bsum[...] = jnp.zeros_like(bsum)
    lsum[...] = jnp.zeros_like(lsum)
    csum[...] = jnp.zeros_like(csum)
    ext[...] = jnp.zeros_like(ext)
    for load in loads[:4]:
        load.wait()

    def prologue(r, carry):
        rows = pl.ds(pl.multiple_of(r * 128, 128), 128)
        length = lens[r // 2]
        place = (r % 2) * 128 + lax.broadcasted_iota(jnp.int32, (128, 128), 0)
        marks = jnp.transpose(jnp.broadcast_to(tgt[pl.ds(r, 1), :].astype(F32), (128, 128)))
        chosen = ((marks == 1.0) | (place == length - 1)) & (place < length)
        flag = jnp.where(chosen, 1.0, 0.0)
        csum[...] += jnp.sum(flag, axis=0, keepdims=True)
        wide = jnp.concatenate([flag] * 8, axis=1)
        cot[rows, :] = jnp.where(wide > 0.0, lab[rows, :].astype(F32), 0.0).astype(BF16)
        center, inv = row_stats(tok[rows, :].astype(F32))
        y = center * inv
        normed[rows, :] = y.astype(BF16)
        normed_t[:, rows] = jnp.transpose(y).astype(BF16)
        return carry

    lax.fori_loop(0, 4, prologue, 0)
    loads[4].wait()
    loads[5].wait()

    for c in range(5):
        cols = slice(c * 512, (c + 1) * 512)
        h = nn(normed[...], win[:, cols]) + wide_row(bias, 4 * c, 4)
        sg = sigmoid(h)
        slope[:, cols] = silu_slope(h, sg).astype(BF16)
        acts[:, cols] = (h * sg).astype(BF16)

    for n in range(2):
        rows = slice(n * LMAX, (n + 1) * LMAX)
        allowed = allowed_mask(lens[n])
        for h in range(HEADS):
            q = acts[rows, D + QCOL + h * QKDIM : D + QCOL + (h + 1) * QKDIM]
            k = acts[rows, D + KCOL + h * QKDIM : D + KCOL + (h + 1) * QKDIM]
            s = nt(q, k)
            sg = sigmoid(s)
            w = jnp.where(allowed, s * sg, 0.0).astype(BF16)
            wt[n * HEADS + h] = w
            ws[n * HEADS + h] = jnp.where(allowed, silu_slope(s, sg), 0.0)
            mixed[rows, h * VDIM : (h + 1) * VDIM] = nn(w, acts[rows, D + h * VDIM : D + (h + 1) * VDIM])

    loads[6].wait()

    def gate(r, carry):
        rows = pl.ds(pl.multiple_of(r * 128, 128), 128)
        center, inv = row_stats(mixed[rows, :])
        y = center * inv
        u = acts[rows, :D].astype(F32)
        gated = (y * u).astype(BF16)
        gated_t[:, rows] = jnp.transpose(gated.astype(F32)).astype(BF16)
        length = lens[r // 2]
        place = (r % 2) * 128 + lax.broadcasted_iota(jnp.int32, (128, D), 0)
        full = tok[rows, :].astype(F32) + nn(gated, wout[...])
        rounded = jnp.where(place < length, full, 0.0).astype(BF16)
        out[rows, :] = rounded
        c = cot[rows, :]
        lsum[...] += jnp.sum(c.astype(F32) * rounded.astype(F32), axis=0, keepdims=True)
        dg = nt(c, wout[...]).astype(BF16).astype(F32)
        dy = dg * u
        du = (dg * y).astype(BF16).astype(F32)
        m1 = jnp.mean(dy, axis=-1, keepdims=True)
        m2 = jnp.mean(dy * y, axis=-1, keepdims=True)
        dm[rows, :] = (inv * (dy - m1 - y * m2)).astype(BF16)
        dhu = du * slope[rows, :D].astype(F32)
        dh[rows, :D] = dhu.astype(BF16)
        bsum[0:1, :D] += jnp.sum(dhu, axis=0, keepdims=True)
        return carry

    lax.fori_loop(0, 4, gate, 0)
    save_out = pltpu.make_async_copy(out, out_hbm, sems.at[7])
    save_out.start()

    for c in range(2):
        g = nn(gated_t[...], cot[:, c * 512 : (c + 1) * 512])
        for i in range(4):
            pack(pay, 20 + 4 * c + i, g[:, i * 128 : (i + 1) * 128])

    for n in range(2):
        rows = slice(n * LMAX, (n + 1) * LMAX)
        for h in range(HEADS):
            q = acts[rows, D + QCOL + h * QKDIM : D + QCOL + (h + 1) * QKDIM]
            k = acts[rows, D + KCOL + h * QKDIM : D + KCOL + (h + 1) * QKDIM]
            vc = slice(D + h * VDIM, D + (h + 1) * VDIM)
            d = dm[rows, h * VDIM : (h + 1) * VDIM]
            dw = nt(d, acts[rows, vc]).astype(BF16).astype(F32)
            dv = tn(wt[n * HEADS + h], d).astype(BF16).astype(F32)
            ds = (dw * ws[n * HEADS + h]).astype(BF16)
            dqk[rows, h * QKDIM : (h + 1) * QKDIM] = nn(ds, k)
            dqk[rows, 256 + h * QKDIM : 256 + (h + 1) * QKDIM] = tn(ds, q)
            dhv = dv * slope[rows, vc].astype(F32)
            dh[rows, vc] = dhv.astype(BF16)
            bsum[0:1, vc] += jnp.sum(dhv, axis=0, keepdims=True)
        dhq = dqk[rows, :].astype(BF16).astype(F32) * slope[rows, 2 * D :].astype(F32)
        dh[rows, 2 * D :] = dhq.astype(BF16)
        bsum[0:1, 2 * D :] += jnp.sum(dhq, axis=0, keepdims=True)

    for c in range(5):
        g = nn(normed_t[...], dh[:, c * 512 : (c + 1) * 512])
        for i in range(4):
            pack(pay, 4 * c + i, g[:, i * 128 : (i + 1) * 128])

    for j in range(COLS // 128):
        parts = three_parts(bsum[0:1, j * 128 : (j + 1) * 128])
        base = 8 * (j // 2) + j % 2
        for t in range(3):
            ext[base + 2 * t : base + 2 * t + 1, :] = parts[t]
    loss = jnp.sum(lsum[...], axis=1, keepdims=True)
    lane = lax.broadcasted_iota(jnp.int32, (1, 128), 1)
    tail = jnp.where(lane == 0, jnp.broadcast_to(loss, (1, 128)), jnp.where(lane == 1, csum[...], 0.0))
    parts = three_parts(tail)
    for t in range(3):
        ext[80 + 2 * t : 81 + 2 * t, :] = parts[t]
    for half in range(2):
        pay[half, 2, :, EXTRA:, :] = jnp.zeros((PIECES, 16, 128), BF16)
        for p in range(11):
            pay[half, 2, p, EXTRA : EXTRA + 8, :] = ext[8 * p : 8 * p + 8, :].astype(BF16)

    moves = [
        pltpu.make_async_copy(pay.at[1 - core, c], ref, sems.at[8 + c])
        for c, ref in enumerate((send_0, send_1, send_2))
    ] + [
        pltpu.make_async_copy(pay.at[core, c], ref, sems.at[11 + c])
        for c, ref in enumerate((mine_0, mine_1, mine_2))
    ]
    for move in moves:
        move.start()

    def back(r, carry):
        rows = pl.ds(pl.multiple_of(r * 128, 128), 128)
        dn = nt(dh[rows, :], win[...]).astype(BF16).astype(F32)
        center, inv = row_stats(tok[rows, :].astype(F32))
        y = center * inv
        m1 = jnp.mean(dn, axis=-1, keepdims=True)
        m2 = jnp.mean(dn * y, axis=-1, keepdims=True)
        dx[rows, :] = inv * (dn - m1 - y * m2) + cot[rows, :].astype(F32)
        return carry

    lax.fori_loop(0, 4, back, 0)
    save_dx = pltpu.make_async_copy(dx, dx_hbm, sems.at[14])
    save_dx.start()
    for copy in [save_out, save_dx] + moves:
        copy.wait()


def local_step(lens, tgt, tok, lab, win, bias, wout):
    third = jax.ShapeDtypeStruct((PIECES, DEEP, 128), BF16)
    wide = pltpu.VMEM((ROWS, COLS), BF16)
    rows = pltpu.VMEM((ROWS, D), BF16)
    turned = pltpu.VMEM((D, ROWS), BF16)
    return pl.pallas_call(
        local_kernel,
        in_specs=[HBM] * 7,
        out_specs=[HBM] * 8,
        out_shape=[jax.ShapeDtypeStruct((ROWS, D), BF16), jax.ShapeDtypeStruct((ROWS, D), F32)] + [third] * 6,
        scratch_shapes=[
            pltpu.SMEM((2,), jnp.int32),
            pltpu.VMEM((4, 128), jnp.int32),
            rows,
            rows,
            pltpu.VMEM((D, COLS), BF16),
            pltpu.VMEM((20, 128), F32),
            pltpu.VMEM((D, D), BF16),
            rows,
            pltpu.VMEM((ROWS, D), F32),
            rows,
            turned,
            wide,
            wide,
            wide,
            pltpu.VMEM((ROWS, D), F32),
            turned,
            rows,
            pltpu.VMEM((2 * HEADS, LMAX, LMAX), BF16),
            pltpu.VMEM((2 * HEADS, LMAX, LMAX), F32),
            rows,
            pltpu.VMEM((ROWS, 512), F32),
            pltpu.VMEM((8, COLS), F32),
            pltpu.VMEM((1, D), F32),
            pltpu.VMEM((1, 128), F32),
            pltpu.VMEM((88, 128), F32),
            pltpu.VMEM((2, COLORS, PIECES, DEEP, 128), BF16),
            pltpu.SemaphoreType.DMA((15,)),
        ],
        compiler_params=pltpu.CompilerParams(vmem_limit_bytes=60 * 2**20),
        name="local_step",
    )(lens, tgt, tok, lab, win, bias, wout)


def resplit(total):
    value = total[..., 0:2, :] + total[..., 2:4, :] + total[..., 4:6, :]
    hi, mid, low = three_parts(value)
    return jnp.concatenate([hi, mid, low, jnp.zeros_like(hi)], axis=-2)


def put_sum(dst, total, extras):
    if extras:
        dst[:, :EXTRA, :] = total[:, :EXTRA, :].astype(BF16)
        dst[:, EXTRA : EXTRA + 8, :] = resplit(total[:, EXTRA : EXTRA + 8, :]).astype(BF16)
        dst[:, EXTRA + 8 :, :] = total[:, EXTRA + 8 :, :].astype(BF16)
    else:
        dst[...] = total.astype(BF16)


def places():
    return [lax.axis_index(a) for a in CHIPS]


CHUNK = (GROUP, DEEP, 128)


def pair_kernel(color, a_hbm, b_hbm, o1, o2, o3, o0, a, b, o, sems):
    outs = {1: o1, 2: o2, 3: o3, 0: o0}
    me = places()[color]

    def load(n, d):
        k = pl.ds(lax.rem(me + d, 4) * GROUP, GROUP)
        return (
            pltpu.make_async_copy(a_hbm.at[k], a.at[n], sems.at[0, n]),
            pltpu.make_async_copy(b_hbm.at[k], b.at[n], sems.at[1, n]),
        )

    order = SHIFTS + (0,)
    for n, d in enumerate(order):
        for copy in load(n, d):
            copy.start()
    saves = []
    for n, d in enumerate(order):
        for copy in load(n, d):
            copy.wait()
        put_sum(o.at[n], a[n].astype(F32) + b[n].astype(F32), color == 2)
        saves.append(pltpu.make_async_copy(o.at[n], outs[d], sems.at[2, n]))
        saves[-1].start()
    for save in saves:
        save.wait()


def pair_add(a, b, color):
    o1, o2, o3, o0 = pl.pallas_call(
        functools.partial(pair_kernel, color),
        in_specs=[ANY, ANY],
        out_specs=[ANY] * 4,
        out_shape=[jax.ShapeDtypeStruct(CHUNK, BF16)] * 4,
        scratch_shapes=[pltpu.VMEM((4,) + CHUNK, BF16)] * 3 + [pltpu.SemaphoreType.DMA((3, 4))],
        compiler_params=pltpu.CompilerParams(vmem_limit_bytes=8 * 2**20),
        name="pair_add",
    )(a, b)
    return {0: o0, 1: o1, 2: o2, 3: o3}


def ring_sum_kernel(axis, extras, *rest):
    ins, (out, buf, o, sems) = rest[:4], rest[4:]
    me = places()[axis]
    copies = [
        pltpu.make_async_copy(ins[d], buf.at[lax.rem(me + 4 - d, 4)], sems.at[d]) for d in range(4)
    ]
    for copy in copies:
        copy.start()
    for copy in copies:
        copy.wait()
    total = (buf[0].astype(F32) + buf[1].astype(F32)) + (buf[2].astype(F32) + buf[3].astype(F32))
    put_sum(o, total, extras)
    save = pltpu.make_async_copy(o, out, sems.at[4])
    save.start()
    save.wait()


def ring_sum(chunks, axis, extras):
    return pl.pallas_call(
        functools.partial(ring_sum_kernel, axis, extras),
        in_specs=[ANY] * 4,
        out_specs=ANY,
        out_shape=jax.ShapeDtypeStruct(CHUNK, BF16),
        scratch_shapes=[
            pltpu.VMEM((4,) + CHUNK, BF16),
            pltpu.VMEM(CHUNK, BF16),
            pltpu.SemaphoreType.DMA((5,)),
        ],
        compiler_params=pltpu.CompilerParams(vmem_limit_bytes=6 * 2**20),
        name="ring_sum",
    )(*[chunks[d] for d in range(4)])


def targets_of(half, color):
    blocks = [half * BLOCKS + jj for jj in range(BLOCKS) if jj // 5 == color]
    low = [j for j in blocks if j < 20]
    high = [j - 20 for j in blocks if j >= 20]
    return low, high


def finish_kernel(*rest):
    ins, dx_hbm = rest[:24], rest[24]
    gin, gout, gtok_hbm, gbias, loss = rest[25:30]
    buf, dx, gtok, vin, vout, sems, outs = rest[30:]
    core = lax.axis_index("c")
    spot = places()
    order = [(s, c, d) for s in range(2) for c in (2, 0, 1) for d in range(4)]

    def load(n):
        s, c, d = order[n]
        return pltpu.make_async_copy(ins[12 * s + 4 * c + d], buf.at[n], sems.at[n])

    load_dx = pltpu.make_async_copy(dx_hbm, dx, sems.at[24])
    for n in range(24):
        load(n).start()
    load_dx.start()
    for n in range(4):
        load(n).wait()
    last = buf[spot[2], 10, EXTRA : EXTRA + 8, :].astype(F32)
    last = last[0:1, :] + last[2:3, :] + last[4:5, :]
    inverse = 1.0 / last[0:1, 1:2]
    loss[...] = last[0:1, 0:1] * inverse
    for p in range(10):
        e = buf[spot[2], p, EXTRA : EXTRA + 8, :].astype(F32)
        gbias[2 * p : 2 * p + 2, :] = (e[0:2, :] + e[2:4, :] + e[4:6, :]) * inverse

    def unpack(half, n):
        _, c, d = order[n]
        base = pl.multiple_of(lax.rem(spot[c] + 4 - d, 4) * 256, 256)
        low, high = targets_of(half, c)
        dests = [(vin, j) for j in low] + [(vout, j) for j in high]

        def piece(q, carry):
            rows = pl.ds(pl.multiple_of(base + q * 16, 16), 16)
            for i, (ref, j) in enumerate(dests):
                value = buf[n, q, i * 16 : (i + 1) * 16, :].astype(F32) * inverse
                ref[rows, j * 128 : (j + 1) * 128] = value.astype(BF16)
            return carry

        lax.fori_loop(0, GROUP, piece, 0)
        copies = []
        for ref, dst, blocks, k in ((vin, gin, low, 0), (vout, gout, high, 1)):
            if blocks:
                window = (pl.ds(base, 256), pl.ds(blocks[0] * 128, len(blocks) * 128))
                copies.append(pltpu.make_async_copy(ref.at[window], dst.at[window], outs.at[k, n]))
        return copies

    def run(me):
        saves = []
        for n in range(24):
            if n >= 4:
                load(n).wait()
            copies = unpack(me if order[n][0] == 0 else 1 - me, n)
            for copy in copies:
                copy.start()
            saves += copies
        for save in saves:
            save.wait()

    @pl.when(core == 0)
    def _():
        run(0)

    @pl.when(core == 1)
    def _():
        run(1)

    load_dx.wait()
    gtok[...] = (dx[...] * inverse).astype(BF16)
    save = pltpu.make_async_copy(gtok, gtok_hbm, sems.at[25])
    save.start()
    save.wait()


def finish(chunks, dx):
    return pl.pallas_call(
        finish_kernel,
        in_specs=[ANY] * 24 + [HBM],
        out_specs=[HBM, HBM, HBM, VM, VM],
        out_shape=[
            jax.ShapeDtypeStruct((D, COLS), BF16),
            jax.ShapeDtypeStruct((D, D), BF16),
            jax.ShapeDtypeStruct((ROWS, D), BF16),
            jax.ShapeDtypeStruct((20, 128), F32),
            jax.ShapeDtypeStruct((1, 1), F32),
        ],
        scratch_shapes=[
            pltpu.VMEM((24,) + CHUNK, BF16),
            pltpu.VMEM((ROWS, D), F32),
            pltpu.VMEM((ROWS, D), BF16),
            pltpu.VMEM((D, COLS), BF16),
            pltpu.VMEM((D, D), BF16),
            pltpu.SemaphoreType.DMA((26,)),
            pltpu.SemaphoreType.DMA((2, 24)),
        ],
        compiler_params=pltpu.CompilerParams(vmem_limit_bytes=28 * 2**20),
        name="finish",
    )(*chunks, dx)


def swap(value):
    return lax.ppermute(value, "c", [(0, 1), (1, 0)])


def shift(value, axis, d):
    return lax.ppermute(value, CHIPS[axis], [(i, (i + d) % 4) for i in range(4)])


def shards(tokens, labels, lengths, targets, w_in, b_in, w_out):
    out, dx, *thirds = local_step(
        lengths, targets.reshape(4, 128), tokens, labels, w_in, b_in.reshape(20, 128), w_out
    )
    swapped = [swap(third) for third in thirds[3:]]
    colors = range(COLORS)
    value = []
    for c in colors:
        chunks = pair_add(thirds[c], swapped[c], c)
        for d in SHIFTS:
            chunks[d] = shift(chunks[d], TURNS[c][0], d)
        value.append(chunks)
    value = [ring_sum(value[c], TURNS[c][0], c == 2) for c in colors]
    for turn in (1, 2):
        for c in colors:
            chunks = {0: value[c]}
            for d in SHIFTS:
                chunks[d] = shift(value[c], TURNS[c][turn], d)
            value[c] = ring_sum(chunks, TURNS[c][turn], c == 2)
    own = {}
    for c in colors:
        own[c, 0] = value[c]
        for d in SHIFTS:
            own[c, d] = shift(value[c], TURNS[c][0], d)
    keys = [(c, d) for c in colors for d in range(4)]
    other = {key: swap(own[key]) for key in keys}
    gin, gout, gtok, gbias, loss = finish([own[k] for k in keys] + [other[k] for k in keys], dx)
    return out, loss.reshape(()), gtok, gin, gbias.reshape(COLS), gout


def solution(mesh):
    torus = Mesh(mesh.devices.reshape(4, 4, 4, 2), AXES)
    placed = (P(AXES, None), P(AXES, None), P(AXES), P(AXES), P(), P(), P())
    return jax.shard_map(
        shards,
        mesh=torus,
        in_specs=placed,
        out_specs=(P(AXES, None), P(), P(AXES, None), P(), P(), P()),
        check_vma=False,
    )
```

```python
import functools

import jax
import jax.numpy as jnp
from jax import lax
from jax.experimental import pallas as pl
from jax.experimental.pallas import tpu as pltpu
from jax.sharding import Mesh
from jax.sharding import PartitionSpec as P

D = 1024
HEADS = 4
VDIM = 256
QKDIM = 64
LMAX = 256
COLS = 2560
REST = 1536
ROWS = 512
QCOL = 1024
KCOL = 1280
AXES = ("z", "x", "y", "c")
CHIPS = ("z", "x", "y")
TURNS = ((0, 1, 2), (1, 2, 0), (2, 0, 1))
NEAR = [(0, 1), (1, 0), (2, 3), (3, 2)]
FAR = [(0, 3), (3, 0), (1, 2), (2, 1)]
PIECES = 64
BLOCKS = 14
COLORS = 3
DEEP = 80
EXTRA = 64
GROUP = 16
EPS = 1e-05
F32 = jnp.float32
BF16 = jnp.bfloat16
VM = pl.BlockSpec(memory_space=pltpu.VMEM)
SM = pl.BlockSpec(memory_space=pltpu.SMEM)
HBM = pl.BlockSpec(memory_space=pltpu.HBM)
ANY = pl.BlockSpec(memory_space=pl.ANY)


def cost(flops):
    return pl.CostEstimate(flops=flops, transcendentals=0, bytes_accessed=8 * 2**20)


def sigmoid(h):
    return 0.5 * jnp.tanh(0.5 * h) + 0.5


def silu_slope(h, sg):
    return sg * (1.0 + h * (1.0 - sg))


def nn(a, b):
    return jnp.dot(a, b, preferred_element_type=F32)


def nt(a, b):
    return lax.dot_general(a, b, (((1,), (1,)), ((), ())), preferred_element_type=F32)


def tn(a, b):
    return lax.dot_general(a, b, (((0,), (0,)), ((), ())), preferred_element_type=F32)


def three_parts(value):
    hi = value.astype(BF16).astype(F32)
    rest = value - hi
    mid = rest.astype(BF16).astype(F32)
    low = (rest - mid).astype(BF16).astype(F32)
    return hi, mid, low


def row_stats(x):
    center = x - jnp.mean(x, axis=-1, keepdims=True)
    spread = jnp.mean(center * center, axis=-1, keepdims=True)
    return center, lax.rsqrt(spread + EPS)


def allowed_mask(length):
    i = lax.broadcasted_iota(jnp.int32, (LMAX, LMAX), 0)
    j = lax.broadcasted_iota(jnp.int32, (LMAX, LMAX), 1)
    return (j <= i) & (j < length)


def wide_row(ref, first, count):
    return jnp.concatenate([ref[j : j + 1, :] for j in range(first, first + count)], axis=1)


def pack(pay, j, value):
    half, jj = j // BLOCKS, j % BLOCKS
    color, row = (jj // 5 + 1) % 3, (jj % 5) * 16
    pay[half, color, :, row : row + 16, :] = value.astype(BF16).reshape(PIECES, 16, 128)


def local_kernel(
    lens_hbm, tgt_hbm, tok_hbm, lab_hbm, win_hbm, bias_hbm, wout_hbm,
    out_hbm, dx_hbm, mine_0, mine_1, mine_2, send_0, send_1, send_2,
    lens, tgt, tok, lab, win, bias, wout, out, dx,
    normed, normed_t, slope, acts, dh, mixed, gated_t, dm, wt, ws, cot, dqk, bsum, lsum, csum, ext, pay, sems,
):
    core = lax.axis_index("c")
    pairs = (
        (lens_hbm, lens), (tgt_hbm, tgt), (tok_hbm, tok), (lab_hbm, lab),
        (win_hbm, win), (bias_hbm, bias), (wout_hbm, wout),
    )
    loads = [pltpu.make_async_copy(a, b, sems.at[n]) for n, (a, b) in enumerate(pairs)]
    for load in loads:
        load.start()
    bsum[...] = jnp.zeros_like(bsum)
    lsum[...] = jnp.zeros_like(lsum)
    csum[...] = jnp.zeros_like(csum)
    ext[...] = jnp.zeros_like(ext)
    for load in loads[:4]:
        load.wait()

    def prologue(r, carry):
        rows = pl.ds(pl.multiple_of(r * 128, 128), 128)
        length = lens[r // 2]
        place = (r % 2) * 128 + lax.broadcasted_iota(jnp.int32, (128, 128), 0)
        marks = jnp.transpose(jnp.broadcast_to(tgt[pl.ds(r, 1), :].astype(F32), (128, 128)))
        chosen = ((marks == 1.0) | (place == length - 1)) & (place < length)
        flag = jnp.where(chosen, 1.0, 0.0)
        csum[...] += jnp.sum(flag, axis=0, keepdims=True)
        wide = jnp.concatenate([flag] * 8, axis=1)
        cot[rows, :] = jnp.where(wide > 0.0, lab[rows, :].astype(F32), 0.0).astype(BF16)
        center, inv = row_stats(tok[rows, :].astype(F32))
        y = center * inv
        normed[rows, :] = y.astype(BF16)
        normed_t[:, rows] = jnp.transpose(y).astype(BF16)
        return carry

    lax.fori_loop(0, 4, prologue, 0)
    loads[4].wait()
    loads[5].wait()

    for c in range(5):
        cols = slice(c * 512, (c + 1) * 512)
        h = nn(normed[...], win[:, cols]) + wide_row(bias, 4 * c, 4)
        sg = sigmoid(h)
        slope[:, cols] = silu_slope(h, sg).astype(BF16)
        acts[:, cols] = (h * sg).astype(BF16)

    for n in range(2):
        rows = slice(n * LMAX, (n + 1) * LMAX)
        allowed = allowed_mask(lens[n])
        for h in range(HEADS):
            q = acts[rows, D + QCOL + h * QKDIM : D + QCOL + (h + 1) * QKDIM]
            k = acts[rows, D + KCOL + h * QKDIM : D + KCOL + (h + 1) * QKDIM]
            s = nt(q, k)
            sg = sigmoid(s)
            w = jnp.where(allowed, s * sg, 0.0).astype(BF16)
            wt[n * HEADS + h] = w
            ws[n * HEADS + h] = jnp.where(allowed, silu_slope(s, sg), 0.0)
            mixed[rows, h * VDIM : (h + 1) * VDIM] = nn(w, acts[rows, D + h * VDIM : D + (h + 1) * VDIM])

    loads[6].wait()

    def gate(r, carry):
        rows = pl.ds(pl.multiple_of(r * 128, 128), 128)
        center, inv = row_stats(mixed[rows, :])
        y = center * inv
        u = acts[rows, :D].astype(F32)
        gated = (y * u).astype(BF16)
        gated_t[:, rows] = jnp.transpose(gated.astype(F32)).astype(BF16)
        length = lens[r // 2]
        place = (r % 2) * 128 + lax.broadcasted_iota(jnp.int32, (128, D), 0)
        full = tok[rows, :].astype(F32) + nn(gated, wout[...])
        rounded = jnp.where(place < length, full, 0.0).astype(BF16)
        out[rows, :] = rounded
        c = cot[rows, :]
        lsum[...] += jnp.sum(c.astype(F32) * rounded.astype(F32), axis=0, keepdims=True)
        dg = nt(c, wout[...]).astype(BF16).astype(F32)
        dy = dg * u
        du = (dg * y).astype(BF16).astype(F32)
        m1 = jnp.mean(dy, axis=-1, keepdims=True)
        m2 = jnp.mean(dy * y, axis=-1, keepdims=True)
        dm[rows, :] = (inv * (dy - m1 - y * m2)).astype(BF16)
        dhu = du * slope[rows, :D].astype(F32)
        dh[rows, :D] = dhu.astype(BF16)
        bsum[0:1, :D] += jnp.sum(dhu, axis=0, keepdims=True)
        return carry

    lax.fori_loop(0, 4, gate, 0)
    save_out = pltpu.make_async_copy(out, out_hbm, sems.at[7])
    save_out.start()

    for c in range(2):
        g = nn(gated_t[...], cot[:, c * 512 : (c + 1) * 512])
        for i in range(4):
            pack(pay, 20 + 4 * c + i, g[:, i * 128 : (i + 1) * 128])

    for n in range(2):
        rows = slice(n * LMAX, (n + 1) * LMAX)
        for h in range(HEADS):
            q = acts[rows, D + QCOL + h * QKDIM : D + QCOL + (h + 1) * QKDIM]
            k = acts[rows, D + KCOL + h * QKDIM : D + KCOL + (h + 1) * QKDIM]
            vc = slice(D + h * VDIM, D + (h + 1) * VDIM)
            d = dm[rows, h * VDIM : (h + 1) * VDIM]
            dw = nt(d, acts[rows, vc]).astype(BF16).astype(F32)
            dv = tn(wt[n * HEADS + h], d).astype(BF16).astype(F32)
            ds = (dw * ws[n * HEADS + h]).astype(BF16)
            dqk[rows, h * QKDIM : (h + 1) * QKDIM] = nn(ds, k)
            dqk[rows, 256 + h * QKDIM : 256 + (h + 1) * QKDIM] = tn(ds, q)
            dhv = dv * slope[rows, vc].astype(F32)
            dh[rows, vc] = dhv.astype(BF16)
            bsum[0:1, vc] += jnp.sum(dhv, axis=0, keepdims=True)
        dhq = dqk[rows, :].astype(BF16).astype(F32) * slope[rows, 2 * D :].astype(F32)
        dh[rows, 2 * D :] = dhq.astype(BF16)
        bsum[0:1, 2 * D :] += jnp.sum(dhq, axis=0, keepdims=True)

    for c in range(5):
        g = nn(normed_t[...], dh[:, c * 512 : (c + 1) * 512])
        for i in range(4):
            pack(pay, 4 * c + i, g[:, i * 128 : (i + 1) * 128])

    for j in range(COLS // 128):
        parts = three_parts(bsum[0:1, j * 128 : (j + 1) * 128])
        base = 8 * (j // 2) + j % 2
        for t in range(3):
            ext[base + 2 * t : base + 2 * t + 1, :] = parts[t]
    loss = jnp.sum(lsum[...], axis=1, keepdims=True)
    lane = lax.broadcasted_iota(jnp.int32, (1, 128), 1)
    tail = jnp.where(lane == 0, jnp.broadcast_to(loss, (1, 128)), jnp.where(lane == 1, csum[...], 0.0))
    parts = three_parts(tail)
    for t in range(3):
        ext[80 + 2 * t : 81 + 2 * t, :] = parts[t]
    for half in range(2):
        pay[half, 0, :, EXTRA:, :] = jnp.zeros((PIECES, 16, 128), BF16)
        for p in range(11):
            pay[half, 0, p, EXTRA : EXTRA + 8, :] = ext[8 * p : 8 * p + 8, :].astype(BF16)

    moves = [
        pltpu.make_async_copy(pay.at[1 - core, c], ref, sems.at[8 + c])
        for c, ref in enumerate((send_0, send_1, send_2))
    ] + [
        pltpu.make_async_copy(pay.at[core, c], ref, sems.at[11 + c])
        for c, ref in enumerate((mine_0, mine_1, mine_2))
    ]
    for move in moves:
        move.start()

    def back(r, carry):
        rows = pl.ds(pl.multiple_of(r * 128, 128), 128)
        dn = nt(dh[rows, :], win[...]).astype(BF16).astype(F32)
        center, inv = row_stats(tok[rows, :].astype(F32))
        y = center * inv
        m1 = jnp.mean(dn, axis=-1, keepdims=True)
        m2 = jnp.mean(dn * y, axis=-1, keepdims=True)
        dx[rows, :] = inv * (dn - m1 - y * m2) + cot[rows, :].astype(F32)
        return carry

    lax.fori_loop(0, 4, back, 0)
    save_dx = pltpu.make_async_copy(dx, dx_hbm, sems.at[14])
    save_dx.start()
    for copy in [save_out, save_dx] + moves:
        copy.wait()


def local_step(lens, tgt, tok, lab, win, bias, wout):
    third = jax.ShapeDtypeStruct((PIECES, DEEP, 128), BF16)
    wide = pltpu.VMEM((ROWS, COLS), BF16)
    rows = pltpu.VMEM((ROWS, D), BF16)
    turned = pltpu.VMEM((D, ROWS), BF16)
    return pl.pallas_call(
        local_kernel,
        in_specs=[HBM] * 7,
        out_specs=[HBM] * 8,
        out_shape=[jax.ShapeDtypeStruct((ROWS, D), BF16), jax.ShapeDtypeStruct((ROWS, D), F32)] + [third] * 6,
        scratch_shapes=[
            pltpu.SMEM((2,), jnp.int32),
            pltpu.VMEM((4, 128), jnp.int32),
            rows,
            rows,
            pltpu.VMEM((D, COLS), BF16),
            pltpu.VMEM((20, 128), F32),
            pltpu.VMEM((D, D), BF16),
            rows,
            pltpu.VMEM((ROWS, D), F32),
            rows,
            turned,
            wide,
            wide,
            wide,
            pltpu.VMEM((ROWS, D), F32),
            turned,
            rows,
            pltpu.VMEM((2 * HEADS, LMAX, LMAX), BF16),
            pltpu.VMEM((2 * HEADS, LMAX, LMAX), F32),
            rows,
            pltpu.VMEM((ROWS, 512), F32),
            pltpu.VMEM((8, COLS), F32),
            pltpu.VMEM((1, D), F32),
            pltpu.VMEM((1, 128), F32),
            pltpu.VMEM((88, 128), F32),
            pltpu.VMEM((2, COLORS, PIECES, DEEP, 128), BF16),
            pltpu.SemaphoreType.DMA((15,)),
        ],
        compiler_params=pltpu.CompilerParams(vmem_limit_bytes=60 * 2**20),
        name="local_step",
    )(lens, tgt, tok, lab, win, bias, wout)


def resplit(total):
    value = total[..., 0:2, :] + total[..., 2:4, :] + total[..., 4:6, :]
    hi, mid, low = three_parts(value)
    return jnp.concatenate([hi, mid, low, jnp.zeros_like(hi)], axis=-2)


def put_sum(dst, total, extras):
    if extras:
        dst[:, :EXTRA, :] = total[:, :EXTRA, :].astype(BF16)
        dst[:, EXTRA : EXTRA + 8, :] = resplit(total[:, EXTRA : EXTRA + 8, :]).astype(BF16)
        dst[:, EXTRA + 8 :, :] = total[:, EXTRA + 8 :, :].astype(BF16)
    else:
        dst[...] = total.astype(BF16)


def places():
    return [lax.axis_index(a) for a in CHIPS]


CHUNK = (GROUP, DEEP, 128)


def chunks_of(i):
    near = i + 1 - 2 * lax.rem(i, 2)
    return i, 3 - i, near, 3 - near


def pair_kernel(color, a_hbm, b_hbm, keep, send, a, b, o, sems):
    spots = chunks_of(places()[color])

    def load(n, d):
        k = pl.ds(spots[d] * GROUP, GROUP)
        return (
            pltpu.make_async_copy(a_hbm.at[k], a.at[n], sems.at[0, n]),
            pltpu.make_async_copy(b_hbm.at[k], b.at[n], sems.at[1, n]),
        )

    order = (2, 3, 0, 1)
    for n, d in enumerate(order):
        for copy in load(n, d):
            copy.start()
    saves = []
    for n, d in enumerate(order):
        for copy in load(n, d):
            copy.wait()
        put_sum(o.at[n], a[n].astype(F32) + b[n].astype(F32), color == 0)
        saves.append(pltpu.make_async_copy(o.at[n], (send if n < 2 else keep).at[n % 2], sems.at[2, n]))
        saves[-1].start()
    for save in saves:
        save.wait()


def pair_add(a, b, color):
    return pl.pallas_call(
        functools.partial(pair_kernel, color),
        in_specs=[ANY, ANY],
        out_specs=[ANY] * 2,
        out_shape=[jax.ShapeDtypeStruct((2,) + CHUNK, BF16)] * 2,
        scratch_shapes=[pltpu.VMEM((4,) + CHUNK, BF16)] * 3 + [pltpu.SemaphoreType.DMA((3, 4))],
        compiler_params=pltpu.CompilerParams(vmem_limit_bytes=8 * 2**20),
        name="pair_add",
    )(a, b)


def half_kernel(extras, a, b, keep, send):
    put_sum(send, a[1].astype(F32) + b[1].astype(F32), extras)
    put_sum(keep, a[0].astype(F32) + b[0].astype(F32), extras)


def half_sum(a, b, extras):
    return pl.pallas_call(
        functools.partial(half_kernel, extras),
        in_specs=[VM, VM],
        out_specs=[VM, VM],
        out_shape=[jax.ShapeDtypeStruct(CHUNK, BF16)] * 2,
        compiler_params=pltpu.CompilerParams(vmem_limit_bytes=6 * 2**20),
        name="half_sum",
    )(a, b)


def two_kernel(extras, a, b, o):
    put_sum(o, a[...].astype(F32) + b[...].astype(F32), extras)


def two_sum(a, b, extras):
    return pl.pallas_call(
        functools.partial(two_kernel, extras),
        in_specs=[VM, VM],
        out_specs=VM,
        out_shape=jax.ShapeDtypeStruct(CHUNK, BF16),
        compiler_params=pltpu.CompilerParams(vmem_limit_bytes=4 * 2**20),
        name="two_sum",
    )(a, b)


def targets_of(half, color):
    blocks = [half * BLOCKS + jj for jj in range(BLOCKS) if (jj // 5 + 1) % 3 == color]
    low = [j for j in blocks if j < 20]
    high = [j - 20 for j in blocks if j >= 20]
    return low, high


def unpack_all(color, ins, buf, stage, gin, gout, inverse, sems, outs):
    core = lax.axis_index("c")
    spots = chunks_of(places()[color])
    wide = stage.shape[2]

    def run(me):
        for side in range(2):
            low, high = targets_of(me if side == 0 else 1 - me, color)

            def unpack(d, carry):
                n = side * 4 + d
                spot = jnp.where(d == 0, spots[0], jnp.where(d == 1, spots[1], jnp.where(d == 2, spots[2], spots[3])))

                def piece(q, inner):
                    for i in range(len(low) + len(high)):
                        value = buf[n, q, i * 16 : (i + 1) * 16, :].astype(F32) * inverse
                        stage[n, pl.ds(pl.multiple_of(q * 16, 16), 16), i * 128 : (i + 1) * 128] = value.astype(BF16)
                    return inner

                lax.fori_loop(0, GROUP, piece, 0)
                rows = pl.ds(pl.multiple_of(spot * 256, 256), 256)
                if low:
                    part = stage.at[n, :, pl.ds(0, len(low) * 128)]
                    pltpu.make_async_copy(part, gin.at[rows, pl.ds(low[0] * 128, len(low) * 128)], outs.at[0, n]).start()
                if high:
                    part = stage.at[n, :, pl.ds(len(low) * 128, len(high) * 128)]
                    pltpu.make_async_copy(part, gout.at[rows, pl.ds(high[0] * 128, len(high) * 128)], outs.at[1, n]).start()
                return carry

            for d in range(4):
                pltpu.make_async_copy(ins[side * 4 + d], buf.at[side * 4 + d], sems.at[side * 4 + d]).wait()
            lax.fori_loop(0, 4, unpack, 0)
        for side in range(2):
            low, high = targets_of(me if side == 0 else 1 - me, color)
            for d in range(4):
                n = side * 4 + d
                if low:
                    part = stage.at[n, :, pl.ds(0, len(low) * 128)]
                    pltpu.make_async_copy(part, gin.at[pl.ds(0, 256), pl.ds(low[0] * 128, len(low) * 128)], outs.at[0, n]).wait()
                if high:
                    part = stage.at[n, :, pl.ds(len(low) * 128, len(high) * 128)]
                    pltpu.make_async_copy(part, gout.at[pl.ds(0, 256), pl.ds(high[0] * 128, len(high) * 128)], outs.at[1, n]).wait()

    @pl.when(core == 0)
    def _():
        run(0)

    @pl.when(core == 1)
    def _():
        run(1)


def load_all(ins, buf, sems):
    for n in range(8):
        pltpu.make_async_copy(ins[n], buf.at[n], sems.at[n]).start()


def first_kernel(*rest):
    ins, head, dx_hbm = rest[:8], rest[8], rest[9]
    gin, gout, gtok_hbm, gbias, loss, scale = rest[10:16]
    buf, top, dx, gtok, stage, sems, outs = rest[16:]
    load_all(ins, buf, sems)
    load_dx = pltpu.make_async_copy(dx_hbm, dx, sems.at[8])
    load_dx.start()
    spots = chunks_of(places()[0])
    slot = jnp.where(spots[0] == 0, 0, jnp.where(spots[1] == 0, 1, jnp.where(spots[2] == 0, 2, 3)))
    for d in range(4):
        copy = pltpu.make_async_copy(head[d], top.at[d], sems.at[9 + d])
        copy.start()
        copy.wait()
    last = top[slot, 10, EXTRA : EXTRA + 8, :].astype(F32)
    last = last[0:1, :] + last[2:3, :] + last[4:5, :]
    inverse = 1.0 / last[0:1, 1:2]
    loss[...] = last[0:1, 0:1] * inverse
    scale[...] = jnp.broadcast_to(inverse, (8, 128))
    for p in range(10):
        e = top[slot, p, EXTRA : EXTRA + 8, :].astype(F32)
        gbias[2 * p : 2 * p + 2, :] = (e[0:2, :] + e[2:4, :] + e[4:6, :]) * inverse
    load_dx.wait()
    gtok[...] = (dx[...] * inverse).astype(BF16)
    save = pltpu.make_async_copy(gtok, gtok_hbm, sems.at[13])
    save.start()
    unpack_all(0, ins, buf, stage, gin, gout, inverse, sems, outs)
    save.wait()


def scratch_of(blocks):
    return [
        pltpu.VMEM((8,) + CHUNK, BF16),
        pltpu.VMEM((8, 256, blocks * 128), BF16),
        pltpu.SemaphoreType.DMA((14,)),
        pltpu.SemaphoreType.DMA((2, 8)),
    ]


GIN = jax.ShapeDtypeStruct((D, COLS), BF16)
GOUT = jax.ShapeDtypeStruct((D, D), BF16)


def finish_first(chunks, dx):
    buf, stage, sems, outs = scratch_of(4)

    def kernel(*rest):
        ins, dx_hbm, more = rest[:8], rest[8], rest[9:]
        first_kernel(*ins, ins[:4], dx_hbm, *more)

    return pl.pallas_call(
        kernel,
        in_specs=[ANY] * 8 + [HBM],
        out_specs=[HBM, HBM, HBM, VM, VM, VM],
        out_shape=[
            GIN,
            GOUT,
            jax.ShapeDtypeStruct((ROWS, D), BF16),
            jax.ShapeDtypeStruct((20, 128), F32),
            jax.ShapeDtypeStruct((1, 1), F32),
            jax.ShapeDtypeStruct((8, 128), F32),
        ],
        scratch_shapes=[
            buf,
            pltpu.VMEM((4,) + CHUNK, BF16),
            pltpu.VMEM((ROWS, D), F32),
            pltpu.VMEM((ROWS, D), BF16),
            stage,
            sems,
            outs,
        ],
        compiler_params=pltpu.CompilerParams(vmem_limit_bytes=16 * 2**20),
        name="finish_first",
    )(*chunks, dx)


def finish_next(chunks, scale, gin, gout, color):
    def kernel(*rest):
        ins, (scale_ref, _, _, gin_out, gout_out, buf, stage, sems, outs) = rest[:8], rest[8:]
        load_all(ins, buf, sems)
        unpack_all(color, ins, buf, stage, gin_out, gout_out, scale_ref[0:1, 0:1], sems, outs)

    return pl.pallas_call(
        kernel,
        in_specs=[ANY] * 8 + [VM, HBM, HBM],
        out_specs=[HBM, HBM],
        out_shape=[GIN, GOUT],
        input_output_aliases={9: 0, 10: 1},
        scratch_shapes=scratch_of(5),
        compiler_params=pltpu.CompilerParams(vmem_limit_bytes=12 * 2**20),
        name="finish_next",
    )(*chunks, scale, gin, gout)


def swap(value):
    return lax.ppermute(value, "c", [(0, 1), (1, 0)])


def trade(value, axis, pairs):
    return lax.ppermute(value, CHIPS[axis], pairs)


def shards(tokens, labels, lengths, targets, w_in, b_in, w_out):
    out, dx, *thirds = local_step(
        lengths, targets.reshape(4, 128), tokens, labels, w_in, b_in.reshape(20, 128), w_out
    )
    swapped = [swap(third) for third in thirds[3:]]
    colors = range(COLORS)
    value = []
    for c in colors:
        keep, send = pair_add(thirds[c], swapped[c], c)
        value.append((keep, trade(send, TURNS[c][0], NEAR)))
    for c in colors:
        keep, send = half_sum(*value[c], c == 0)
        value[c] = (keep, trade(send, TURNS[c][0], FAR))
    value = [two_sum(*value[c], c == 0) for c in colors]
    for turn, pairs in ((1, NEAR), (1, FAR), (2, NEAR), (2, FAR)):
        for c in colors:
            value[c] = two_sum(value[c], trade(value[c], TURNS[c][turn], pairs), c == 0)
    chunks = []
    for c in colors:
        far = trade(value[c], TURNS[c][0], FAR)
        near = trade(value[c], TURNS[c][0], NEAR)
        own = [value[c], far, near, trade(far, TURNS[c][0], NEAR)]
        chunks.append(own + [swap(v) for v in own])
    gin, gout, gtok, gbias, loss, scale = finish_first(chunks[0], dx)
    for c in (1, 2):
        gin, gout = finish_next(chunks[c], scale, gin, gout, c)
    return out, loss.reshape(()), gtok, gin, gbias.reshape(COLS), gout


def solution(mesh):
    torus = Mesh(mesh.devices.reshape(4, 4, 4, 2), AXES)
    placed = (P(AXES, None), P(AXES, None), P(AXES), P(AXES), P(), P(), P())
    return jax.shard_map(
        shards,
        mesh=torus,
        in_specs=placed,
        out_specs=(P(AXES, None), P(), P(AXES, None), P(), P(), P()),
        check_vma=False,
    )
```
